256 devices in a mesh: grp: 4 (over x), wide: 64 (over y, z, core).
Axes of the slice: x: 4, y: 4, z: 8, core: 2. Of those that a mesh axis runs over, the one named last changes fastest.
Arguments:
- spectral: float32 [8, 48, 320, 2, 641], P(None, 'grp', 'wide'), may hold values from -0.006 to 0.006
- legendre: float32 [320, 641, 320], P('wide'), may hold values from -18 to 18
- pair_table: int32 [320], replicated, may hold values from 0 to 319, each once
- field_map: int32 [8], replicated, may hold values from 0 to 7, each once
Outputs:
- grid_values: float32 [8, 48, 640, 1280], P('grp', None, 'wide')
- checksums: float32 [8, 48], replicated
The draws below stay inside these ranges and needn't reach their ends.
Inputs may be any that keep to these rules, and one draw needn't show every extreme that they name: Each slot number appears once; slot s holds wavenumbers pair_table[s] and 639 - pair_table[s]. `field_map`: each field appears once.
All inputs are finite; a program needn't handle non-finite values.
Results may differ from the reference program's by a relative error of at most 0.000078.
Values sent between devices are 32-bit elements; how exact they have to be, the bound alone decides.
A program may use at most 256 MiB of HBM per device.

```python
import math
import jax
import jax.numpy as jnp
from jax import lax

WAVES = 640
LAT = 640
LON = 1280
FIELDS = 8
LEVELS = 48
PAIRS = 320
NPAIR = 641


def draw_legendre(key, part):
    base_key = jax.random.fold_in(key, 11)
    row_key = jax.random.fold_in(key, 12)
    dimensions = (WAVES // 2, WAVES + 1, LAT // 2)
    values = jnp.clip(jax.random.normal(base_key, dimensions, jnp.float32), -6.0, 6.0)
    scales = jnp.exp(jax.random.uniform(row_key, (LAT // 2,), jnp.float32, math.log(0.3), math.log(3.0)))
    return values * scales


def shard_levels(stream_key, dims, shards, smallest, high):
    loudness, own = 1.0, jax.random.fold_in(stream_key, 6)
    for dim, shards_of in shards:
        heights = jnp.exp(jax.random.uniform(jax.random.fold_in(own, dim), (shards_of,), jnp.float32, smallest / len(shards), high / len(shards)))
        loudness = loudness * jnp.repeat(heights, dims[dim] // shards_of).reshape([-1 if axis == dim else 1 for axis in range(len(dims))])
    return loudness


def gaussian(key, dims, deviation, bound, shards=(), kind=jnp.bfloat16):
    values = jax.random.normal(key, dims, jnp.float32) * deviation
    if len(shards) > 0:
        values = shard_levels(key, dims, shards, -0.22, 0.18) * values
    return jnp.clip(values, min=-bound, max=bound).astype(kind)


def setup_inputs(seed: int = 0) -> dict:
    streams_of = jax.random.split(jax.random.key(seed), 5)
    return {
        "spectral": gaussian(streams_of[0], (FIELDS, LEVELS, PAIRS, 2, NPAIR), 0.001, 0.006, ((1, 4), (2, 64)), jnp.float32),
        "legendre": draw_legendre(jax.random.fold_in(streams_of[4], 71), 0),
        "pair_table": jax.random.permutation(streams_of[2], PAIRS).astype(jnp.int32),
        "field_map": jax.random.permutation(streams_of[3], FIELDS).astype(jnp.int32),
    }


HIGHEST = lax.Precision.HIGHEST


def parity_masks(slot_pairs):
    degree = jnp.arange(WAVES + 1, dtype=jnp.int32)[None, :]
    boundary = (WAVES - slot_pairs.astype(jnp.int32))[:, None]
    first_part = degree < boundary
    first_even = (degree % 2) == 0
    second_even = ((degree - boundary) % 2) == 0
    stacked = jnp.stack([first_part & first_even, first_part & ~first_even,
                         ~first_part & second_even, ~first_part & ~second_even], 0)
    return stacked.astype(jnp.float32)


def legendre_sums(coeffs, legendre, slot_pairs):
    weights = parity_masks(slot_pairs)
    masked = coeffs[None] * weights[:, None, None, :, None, :]
    summed = jnp.einsum('qflprk,pkh->pqrflh', masked, legendre, precision=HIGHEST)
    even_sums = summed[:, 0::2]
    odd_sums = summed[:, 1::2]
    return jnp.concatenate([even_sums + odd_sums, jnp.flip(even_sums - odd_sums, -1)], -1)


def reference(spectral, legendre, pair_table, field_map):
    ordered = jnp.take(spectral, field_map.astype(jnp.int32), axis=0)
    wavenumber = jnp.stack([pair_table, WAVES - 1 - pair_table], 1).reshape(-1).astype(jnp.int32)

    def one_field(coeffs):
        fourier = legendre_sums(coeffs[None], legendre, pair_table)[:, :, :, 0]
        real_part = jnp.moveaxis(fourier[:, :, 0].reshape(-1, LEVELS, LAT), 0, -1)
        imag_part = jnp.moveaxis(fourier[:, :, 1].reshape(-1, LEVELS, LAT), 0, -1)
        spectrum_real = jnp.zeros((LEVELS, LAT, LON // 2 + 1), jnp.float32).at[:, :, wavenumber].set(real_part)
        spectrum_imag = jnp.zeros((LEVELS, LAT, LON // 2 + 1), jnp.float32).at[:, :, wavenumber].set(imag_part)
        spectrum_imag = spectrum_imag.at[:, :, 0].set(0.0)
        return LON * jnp.fft.irfft(spectrum_real + 1j * spectrum_imag, n=LON, axis=-1)

    grid_values = lax.map(one_field, ordered).astype(jnp.float32)
    checksums = jnp.mean(grid_values * grid_values, axis=(2, 3))
    return grid_values, checksums
```

```python
import functools
import math

import jax
import jax.numpy as jnp
from jax import lax
from jax.experimental import pallas as pl
from jax.experimental.pallas import tpu as pltpu
from jax.sharding import PartitionSpec as P

WAVES = 640
LAT = 640
LON = 1280
HALF = LON // 2
MESH = pl.DeviceIdType.MESH
ROWS = 40
LAST = 32
GROUPS = 4
PEERS = 64


def split(value):
    high = value.astype(jnp.bfloat16)
    low = (value - high.astype(jnp.float32)).astype(jnp.bfloat16)
    return high, low


def kernel(
    pair,
    fields,
    spectral,
    table_hbm,
    table_end,
    pairs_down,
    out,
    sums_out,
    table,
    table_high,
    table_low,
    coeffs_send,
    coeffs,
    waves_send,
    last_send,
    waves,
    last,
    synth_high,
    synth_low,
    left_high,
    left_low,
    energy,
    sums,
    table_sem,
    coeffs_send_sem,
    coeffs_sem,
    waves_send_sem,
    waves_sem,
    sums_send_sem,
    sums_sem,
):
    grp = lax.axis_index("grp")
    wide = lax.axis_index("wide")
    my_y, my_z, my_c = wide // 16, (wide // 2) % 8, wide % 2
    south = wide // 32

    def other_group(step):
        return lax.rem(grp + step, GROUPS)

    def partner(i):
        k = i % 8
        up = (k + 2) // 2
        dz = (k % 2) * (8 - up) + (1 - k % 2) * up
        dz = (1 - k // 6) * dz + (k // 6) * (1 - k % 2) * 4
        dy = 3 - (i // 8) % 4
        dc = 1 - i // 32
        return (
            lax.rem(my_y + dy, 4) * 16 + lax.rem(my_z + dz, 8) * 2 + lax.rem(my_c + dc, 2)
        )

    def block_of(dest):
        return dest + (dest // 32) * (95 - 2 * dest)

    barrier = pltpu.get_barrier_semaphore()
    table_copies = [
        pltpu.make_async_copy(
            table_hbm.at[:, :, tile * 128 : (tile + 1) * 128],
            table.at[tile],
            table_sem.at[tile],
        )
        for tile in range(5)
    ] + [pltpu.make_async_copy(table_end, table.at[5], table_sem.at[5])]
    for copy in table_copies:
        copy.start()

    def greet(i, carry):
        pl.semaphore_signal(
            barrier, inc=1, device_id={"grp": grp, "wide": partner(i)}, device_id_type=MESH
        )
        return carry

    lax.fori_loop(0, PEERS - 1, greet, 0)
    for step in (1, 2, 3):
        pl.semaphore_signal(
            barrier,
            inc=1,
            device_id={"grp": other_group(step), "wide": wide},
            device_id_type=MESH,
        )

    coeffs_send[:, :, :, 640:768] = jnp.zeros((GROUPS, 15, 16, 128), jnp.float32)

    for slot in range(5):

        def reorder(group, carry, slot=slot):
            for j in range(2):
                field = fields[2 * group + j]
                for level in range(12):
                    q, l = level // 4, level % 4
                    block = q * 4 + slot if slot < 4 else 12 + q
                    for c in range(2):
                        coeffs_send[group, block, c * 8 + j * 4 + l, 0:641] = spectral[
                            field, level, slot, c, :
                        ]
            return carry

        lax.fori_loop(0, GROUPS, reorder, 0)

    pl.semaphore_wait(barrier, PEERS - 1 + GROUPS - 1)

    def coeffs_copy(chunk, step):
        blocks = pl.ds(chunk * 4, 4 if chunk < 3 else 3)
        dest = other_group(step)
        return pltpu.make_async_remote_copy(
            src_ref=coeffs_send.at[dest, blocks],
            dst_ref=coeffs.at[grp, blocks],
            send_sem=coeffs_send_sem.at[chunk],
            recv_sem=coeffs_sem.at[chunk],
            device_id={"grp": dest, "wide": wide},
            device_id_type=MESH,
        )

    def coeffs_all(chunk):
        blocks = pl.ds(chunk * 4, 4 if chunk < 3 else 3)
        return pltpu.make_async_remote_copy(
            src_ref=coeffs_send.at[0:3, blocks],
            dst_ref=coeffs.at[0:3, blocks],
            send_sem=coeffs_send_sem.at[chunk],
            recv_sem=coeffs_sem.at[chunk],
            device_id={"grp": other_group(1), "wide": wide},
            device_id_type=MESH,
        )

    for chunk in (0, 1, 3, 2):
        for step in (1, 2, 3):
            coeffs_copy(chunk, step).start()

    def keep_own(block, carry):
        coeffs[grp, block] = coeffs_send[grp, block]
        return carry

    lax.fori_loop(0, 15, keep_own, 0)

    for copy in table_copies:
        copy.wait()

    def part_table(i, carry):
        slot, lat = i // 10, i % 10
        rows = pl.ds(pl.multiple_of(lat * 32, 32), 32)
        for tile in range(6):
            value = table[tile, slot, pl.ds(lat, 32, stride=10), :]
            high, low = split(value)
            table_high[slot, rows, tile * 128 : (tile + 1) * 128] = high
            table_low[slot, rows, tile * 128 : (tile + 1) * 128] = low
        return carry

    lax.fori_loop(0, 50, part_table, 0)

    energy[...] = jnp.zeros_like(energy)
    degree = lax.broadcasted_iota(jnp.int32, (1, 768), 1)
    lane = lax.broadcasted_iota(jnp.int32, (1, 128), 1)

    def legendre(block, slot, q, target, first_row, stride):
        p = pair[wide * 5 + slot]
        boundary = WAVES - p
        first_part = degree < boundary
        start = jnp.where(first_part, 0, boundary)
        sign = 1.0 - 2.0 * ((degree - start) % 2).astype(jnp.float32)
        is_first = first_part.astype(jnp.float32)
        inside = (degree <= WAVES).astype(jnp.float32)
        odd = (p % 2).astype(jnp.float32)
        even_mask = (is_first * (1.0 - odd) + (1.0 - is_first) * odd) * inside
        odd_mask = (1.0 - even_mask) * inside
        x = jnp.concatenate([coeffs[g, block] for g in range(GROUPS)], 0)
        right = jnp.concatenate(
            [x * even_mask, x * odd_mask, x * (even_mask * sign), x * (odd_mask * sign)], 0
        )
        right_high, right_low = split(right)
        nt = (((1,), (1,)), ((), ()))

        def dot(a, b):
            return lax.dot_general(a, b, nt, preferred_element_type=jnp.float32)

        left = table_high[slot]
        result = dot(left, right_high) + dot(left, right_low) + dot(table_low[slot], right_high)
        for lat in range(10):
            rows = result[lat * 32 : (lat + 1) * 32]
            target[pl.ds(first_row + lat, 32, stride=stride), :] = rows[:, 0:128]
            target[pl.ds(first_row + lat + 32 * stride, 32, stride=stride), :] = rows[:, 128:256]
        squares = result * result
        squares = squares[:, 0:128] + squares[:, 128:256]
        total = jnp.sum(squares.reshape(40, 8, 128), axis=0)
        real = 1.0 - ((lane // 8) % 2).astype(jnp.float32)
        zero = jnp.where(p == 0, 1.0, 0.0) * jnp.where(lane < 64, 1.0, 0.0)
        energy[q] = energy[q] + total * (2.0 * (1.0 - zero) + real * zero)

    def wave_copy(chunk, i):
        dest = partner(i)
        size = ROWS if chunk < 3 else LAST
        source = waves_send.at[chunk] if chunk < 3 else last_send
        sink = waves.at[chunk] if chunk < 3 else last
        return pltpu.make_async_remote_copy(
            src_ref=source.at[pl.ds(pl.multiple_of(block_of(dest) * size, 8), size)],
            dst_ref=sink.at[pl.ds(pl.multiple_of(wide * size, 8), size)],
            send_sem=waves_send_sem.at[chunk],
            recv_sem=waves_sem.at[chunk],
            device_id={"grp": grp, "wide": dest},
            device_id_type=MESH,
        )

    def wave_all(chunk):
        size = ROWS if chunk < 3 else LAST
        source = waves_send.at[chunk] if chunk < 3 else last_send
        sink = waves.at[chunk] if chunk < 3 else last
        return pltpu.make_async_remote_copy(
            src_ref=source.at[pl.ds(0, (PEERS - 1) * size)],
            dst_ref=sink.at[pl.ds(0, (PEERS - 1) * size)],
            send_sem=waves_send_sem.at[chunk],
            recv_sem=waves_sem.at[chunk],
            device_id={"grp": grp, "wide": partner(0)},
            device_id_type=MESH,
        )

    def send_waves(chunk):
        def one(i, carry):
            wave_copy(chunk, i).start()
            return carry

        lax.fori_loop(0, PEERS - 1, one, 0)
        size = ROWS if chunk < 3 else LAST
        source = waves_send.at[chunk] if chunk < 3 else last_send
        sink = waves.at[chunk] if chunk < 3 else last
        sink[pl.ds(pl.multiple_of(wide * size, 8), size), :] = source[
            pl.ds(pl.multiple_of(block_of(wide) * size, 8), size), :
        ]

    def legendre_chunk(q):
        coeffs_all(q).wait_recv()

        def one(slot, carry):
            legendre(q * 4 + slot, slot, q, waves_send.at[q], slot * 10, ROWS)
            return carry

        lax.fori_loop(0, 4, one, 0)

    legendre_chunk(0)
    send_waves(0)
    legendre_chunk(1)
    send_waves(1)
    coeffs_all(3).wait_recv()

    def last_slot(q, carry):
        legendre(12 + q, 4, q, last_send, q * 10, LAST)
        return carry

    lax.fori_loop(0, 3, last_slot, 0)
    legendre_chunk(2)

    def folded(q):
        row = jnp.sum(energy[q], axis=0, keepdims=True)
        row = row + pltpu.roll(row, 64, 1)
        low_part = (lane // 8) % 2 == 0
        return row + jnp.where(low_part, pltpu.roll(row, 120, 1), pltpu.roll(row, 8, 1))

    shares = jnp.where(
        lane < 64, jnp.where((lane // 8) % 2 == 0, folded(0), folded(1)), folded(2)
    )
    shares = jnp.broadcast_to(shares, (64, 128))
    last_send[pl.ds(30, 64, stride=LAST), :] = shares
    last_send[pl.ds(31, 64, stride=LAST), :] = shares
    send_waves(3)
    send_waves(2)

    def cosine(phase):
        phase = phase - LON * jnp.floor(phase * (1.0 / LON) + 0.5)
        angle = (LON // 4 - jnp.abs(phase)) * (2.0 * math.pi / LON)
        square = angle * angle
        series = 1.0 / 6227020800.0
        for term in (-1.0 / 39916800.0, 1.0 / 362880.0, -1.0 / 5040.0, 1.0 / 120.0, -1.0 / 6.0, 1.0):
            series = series * square + term
        return series * angle

    column = lax.broadcasted_iota(jnp.int32, (64, 128), 1)

    def make_synthesis(i, carry):
        parity, slot = i // 5, i % 5
        p = pairs_down[pl.ds(pl.multiple_of(slot * 64, 64), 64), :]
        number = jnp.where(p % 2 == parity, p, WAVES - 1 - p)
        factor = jnp.where(number == 0, 1.0, 2.0)
        cos_row = pl.multiple_of(slot * 64 + (slot // 4) * 256, 64)
        sin_row = pl.multiple_of(256 + slot * 64 + (slot // 4) * 64, 64)
        for tile in range(5):
            phase = (number * (column + tile * 128)).astype(jnp.float32)
            lanes = pl.ds(tile * 128, 128)
            high, low = split(factor * cosine(phase))
            synth_high[parity, pl.ds(cos_row, 64), lanes] = high
            synth_low[parity, pl.ds(cos_row, 64), lanes] = low
            high, low = split(-factor * cosine(phase - LON // 4))
            synth_high[parity, pl.ds(sin_row, 64), lanes] = high
            synth_low[parity, pl.ds(sin_row, 64), lanes] = low
        return carry

    lax.fori_loop(0, 10, make_synthesis, 0)

    def synthesis(q):
        def turn(lat, carry):
            main = jnp.concatenate(
                [waves[q, pl.ds(s * 10 + lat, 64, stride=ROWS), :] for s in range(4)], 0
            )
            main = main.T.reshape(2, 4, 2, 8, 256)
            rest = last[pl.ds(q * 10 + lat, 64, stride=LAST), :].T.reshape(2, 4, 2, 8, 64)
            rows = pl.ds(pl.multiple_of(lat * 32, 32), 32)
            for parity in range(2):
                for c in range(2):
                    high, low = split(main[parity, :, c].reshape(32, 256))
                    left_high[parity, rows, c * 256 : (c + 1) * 256] = high
                    left_low[parity, rows, c * 256 : (c + 1) * 256] = low
                high, low = split(
                    jnp.concatenate(
                        [rest[parity, :, 0].reshape(32, 64), rest[parity, :, 1].reshape(32, 64)], 1
                    )
                )
                left_high[parity, rows, 512:640] = high
                left_low[parity, rows, 512:640] = low
            return carry

        lax.fori_loop(0, 10, turn, 0)

        def dot(a, b):
            return jnp.dot(a, b, preferred_element_type=jnp.float32)

        for start, width in ((0, 256), (256, 256), (512, 128)):
            halves = []
            for parity in range(2):
                right_high = synth_high[parity, :, start : start + width]
                right_low = synth_low[parity, :, start : start + width]
                halves.append(
                    dot(left_high[parity], right_high)
                    + dot(left_high[parity], right_low)
                    + dot(left_low[parity], right_high)
                )
            for value, offset in ((halves[0] + halves[1], 0), (halves[0] - halves[1], HALF)):
                for lat in range(10):
                    place = lat + south * (9 - 2 * lat)
                    for g in range(GROUPS):
                        for j in range(2):
                            row = lat * 32 + g * 8 + j * 4
                            level = g * 12 + q * 4
                            out[
                                j,
                                place,
                                level : level + 4,
                                offset + start : offset + start + width,
                            ] = value[row : row + 4]

    wave_all(0).wait_recv()
    wave_all(1).wait_recv()
    wave_all(3).wait_recv()

    total = jnp.sum(last[pl.ds(30, 64, stride=LAST), :], axis=0, keepdims=True)
    sums[grp] = jnp.broadcast_to(total, (8, 128))

    def sums_copy(step):
        dest = other_group(step)
        return pltpu.make_async_remote_copy(
            src_ref=sums.at[grp],
            dst_ref=sums.at[grp],
            send_sem=sums_send_sem,
            recv_sem=sums_sem,
            device_id={"grp": dest, "wide": wide},
            device_id_type=MESH,
        )

    synthesis(0)
    for step in (1, 2, 3):
        sums_copy(step).start()
    synthesis(1)
    sums_all = pltpu.make_async_remote_copy(
        src_ref=sums.at[0:3],
        dst_ref=sums.at[0:3],
        send_sem=sums_send_sem,
        recv_sem=sums_sem,
        device_id={"grp": other_group(1), "wide": wide},
        device_id_type=MESH,
    )
    sums_all.wait_send()
    sums_all.wait_recv()
    sums_out[...] = sums[...]
    wave_all(2).wait_recv()
    synthesis(2)
    for chunk in range(4):
        coeffs_all(chunk).wait_send()
        wave_all(chunk).wait_send()


def local(spectral, legendre, pair_table, field_map):
    table = jnp.swapaxes(legendre, 1, 2)
    table_end = jnp.pad(table[:, :, 640:641], ((0, 0), (0, 0), (0, 127)))
    by_slot = pair_table.reshape(PEERS, 5).T.reshape(-1, 1)
    pairs_down = jnp.broadcast_to(by_slot, (320, 128))
    smem = pl.BlockSpec(memory_space=pltpu.SMEM)
    vmem = pl.BlockSpec(memory_space=pltpu.VMEM)
    anywhere = pl.BlockSpec(memory_space=pl.ANY)
    dma = pltpu.SemaphoreType.DMA
    grid, sums = pl.pallas_call(
        kernel,
        name="transform",
        out_shape=(
            jax.ShapeDtypeStruct((2, 10, 48, LON), jnp.float32),
            jax.ShapeDtypeStruct((GROUPS, 8, 128), jnp.float32),
        ),
        in_specs=[smem, smem, vmem, anywhere, anywhere, vmem],
        out_specs=(vmem, vmem),
        scratch_shapes=[
            pltpu.VMEM((6, 5, 320, 128), jnp.float32),
            pltpu.VMEM((5, 320, 768), jnp.bfloat16),
            pltpu.VMEM((5, 320, 768), jnp.bfloat16),
            pltpu.VMEM((GROUPS, 15, 16, 768), jnp.float32),
            pltpu.VMEM((GROUPS, 15, 16, 768), jnp.float32),
            pltpu.VMEM((3, PEERS * ROWS, 128), jnp.float32),
            pltpu.VMEM((PEERS * LAST, 128), jnp.float32),
            pltpu.VMEM((3, PEERS * ROWS, 128), jnp.float32),
            pltpu.VMEM((PEERS * LAST, 128), jnp.float32),
            pltpu.VMEM((2, HALF, HALF), jnp.bfloat16),
            pltpu.VMEM((2, HALF, HALF), jnp.bfloat16),
            pltpu.VMEM((2, 320, HALF), jnp.bfloat16),
            pltpu.VMEM((2, 320, HALF), jnp.bfloat16),
            pltpu.VMEM((3, 8, 128), jnp.float32),
            pltpu.VMEM((GROUPS, 8, 128), jnp.float32),
            dma((6,)),
            dma((4,)),
            dma((4,)),
            dma((4,)),
            dma((4,)),
            dma,
            dma,
        ],
        compiler_params=pltpu.CompilerParams(
            collective_id=0, has_side_effects=True, vmem_limit_bytes=58 * 2**20
        ),
    )(pair_table, field_map, spectral, table, table_end, pairs_down)
    grid = jnp.swapaxes(grid, 1, 2)
    by_part = sums[:, 0, :].reshape(GROUPS, 2, 4, 2, 2, 4)
    chunks = jnp.stack([by_part[:, 0, :, 0], by_part[:, 0, :, 1], by_part[:, 1, :, 0]], 1)
    checksums = jnp.transpose(chunks, (0, 3, 2, 1, 4)).reshape(8, 48) * (1.0 / LAT)
    return grid, checksums


def solution(mesh):
    placed = (P(None, "grp", "wide", None, None), P("wide", None, None), P(), P())
    return jax.shard_map(
        local,
        mesh=mesh,
        in_specs=placed,
        out_specs=(P("grp", None, "wide", None), P()),
        check_vma=False,
    )
```

```python
import functools
import math

import jax
import jax.numpy as jnp
from jax import lax
from jax.experimental import pallas as pl
from jax.experimental.pallas import tpu as pltpu
from jax.sharding import PartitionSpec as P

WAVES = 640
LAT = 640
LON = 1280
HALF = LON // 2
MESH = pl.DeviceIdType.MESH
ROWS = 40
LAST = 32
GROUPS = 4
PEERS = 64


def split(value):
    high = value.astype(jnp.bfloat16)
    low = (value - high.astype(jnp.float32)).astype(jnp.bfloat16)
    return high, low


def kernel(
    pair,
    fields,
    spectral,
    table_hbm,
    out,
    sums_out,
    table_whole,
    table,
    pairs_down,
    table_high,
    table_low,
    coeffs_send,
    coeffs,
    waves_send,
    last_send,
    waves,
    last,
    synth_high,
    synth_low,
    left_high,
    left_low,
    left,
    energy,
    shares_send,
    shares,
    sums,
    table_sem,
    coeffs_send_sem,
    coeffs_sem,
    waves_send_sem,
    waves_sem,
    shares_send_sem,
    shares_sem,
    sums_send_sem,
    sums_sem,
):
    grp = lax.axis_index("grp")
    wide = lax.axis_index("wide")
    my_y, my_z, my_c = wide // 16, (wide // 2) % 8, wide % 2
    south = wide // 32

    def other_group(step):
        return lax.rem(grp + step, GROUPS)

    def partner(i):
        k = i % 8
        up = (k + 2) // 2
        dz = (k % 2) * (8 - up) + (1 - k % 2) * up
        dz = (1 - k // 6) * dz + (k // 6) * (1 - k % 2) * 4
        dy = 3 - (i // 8) % 4
        dc = 1 - i // 32
        return (
            lax.rem(my_y + dy, 4) * 16 + lax.rem(my_z + dz, 8) * 2 + lax.rem(my_c + dc, 2)
        )

    def block_of(dest):
        return dest + (dest // 32) * (95 - 2 * dest)

    barrier = pltpu.get_barrier_semaphore()
    table_copies = [
        pltpu.make_async_copy(
            table_hbm.at[:, :, tile * 128 : (tile + 1) * 128],
            table.at[tile],
            table_sem.at[tile],
        )
        for tile in range(5)
    ] + [pltpu.make_async_copy(table_hbm, table_whole, table_sem.at[5])]
    for copy in table_copies:
        copy.start()

    def greet(i, carry):
        pl.semaphore_signal(
            barrier, inc=1, device_id={"grp": grp, "wide": partner(i)}, device_id_type=MESH
        )
        return carry

    lax.fori_loop(0, PEERS - 1, greet, 0)
    for step in (1, 2, 3):
        pl.semaphore_signal(
            barrier,
            inc=1,
            device_id={"grp": other_group(step), "wide": wide},
            device_id_type=MESH,
        )

    coeffs_send[:, :, :, 640:768] = jnp.zeros((GROUPS, 15, 16, 128), jnp.float32)

    def reorder(i, carry):
        group, slot = lax.rem(grp + i // 5, GROUPS), i % 5
        for j in range(2):
            field = fields[2 * group + j]
            for level in range(12):
                q, l = level // 4, level % 4
                for c in range(2):
                    coeffs_send[group, q * 5 + slot, c * 8 + j * 4 + l, 0:641] = spectral[
                        field, level, slot, c, :
                    ]
        return carry

    lax.fori_loop(0, 5, reorder, 0)

    def coeffs_copy(chunk, step):
        blocks = pl.ds(chunk * 5, 5)
        dest = other_group(step)
        return pltpu.make_async_remote_copy(
            src_ref=coeffs_send.at[dest, blocks],
            dst_ref=coeffs.at[grp, blocks],
            send_sem=coeffs_send_sem.at[chunk],
            recv_sem=coeffs_sem.at[chunk],
            device_id={"grp": dest, "wide": wide},
            device_id_type=MESH,
        )

    def coeffs_all(chunk):
        blocks = pl.ds(chunk * 5, 5)
        return pltpu.make_async_remote_copy(
            src_ref=coeffs_send.at[0:3, blocks],
            dst_ref=coeffs.at[0:3, blocks],
            send_sem=coeffs_send_sem.at[chunk],
            recv_sem=coeffs_sem.at[chunk],
            device_id={"grp": other_group(1), "wide": wide},
            device_id_type=MESH,
        )

    for copy in table_copies:
        copy.wait()
    first_lane = lax.broadcasted_iota(jnp.int32, (320, 128), 1) == 0

    def part_end(slot, carry):
        table[5, slot] = jnp.where(first_lane, table_whole[slot, :, 640:641], 0.0)
        return carry

    lax.fori_loop(0, 5, part_end, 0)

    def part_table(i, carry):
        slot, lat = i // 10, i % 10
        rows = pl.ds(pl.multiple_of(lat * 32, 32), 32)
        for tile in range(6):
            value = table[tile, slot, pl.ds(lat, 32, stride=10), :]
            high, low = split(value)
            table_high[slot, rows, tile * 128 : (tile + 1) * 128] = high
            table_low[slot, rows, tile * 128 : (tile + 1) * 128] = low
        return carry

    lax.fori_loop(0, 50, part_table, 0)

    energy[...] = jnp.zeros_like(energy)
    degree = lax.broadcasted_iota(jnp.int32, (1, 768), 1)
    lane = lax.broadcasted_iota(jnp.int32, (1, 128), 1)

    def masks(slot):
        p = pair[wide * 5 + slot]
        boundary = WAVES - p
        first_part = degree < boundary
        start = jnp.where(first_part, 0, boundary)
        sign = 1.0 - 2.0 * ((degree - start) % 2).astype(jnp.float32)
        is_first = first_part.astype(jnp.float32)
        inside = (degree <= WAVES).astype(jnp.float32)
        odd = (p % 2).astype(jnp.float32)
        even_mask = (is_first * (1.0 - odd) + (1.0 - is_first) * odd) * inside
        odd_mask = (1.0 - even_mask) * inside
        return p, even_mask, odd_mask, sign

    def piece(dx, q, slot):
        if dx is None:
            return coeffs_send[grp, q * 5 + slot]
        return coeffs[lax.rem(grp + dx, GROUPS), q * 5 + slot]

    nt = (((1,), (1,)), ((), ()))

    def dot_nt(a, b):
        return lax.dot_general(a, b, nt, preferred_element_type=jnp.float32)

    def wave_row(slots, members, tiles, groups, target, first_row, stride):
        result = None
        zero = jnp.zeros((1, 128), jnp.float32)
        empty = jnp.zeros((32, 768), jnp.float32)
        for number, slot in enumerate(slots):
            p, even_mask, odd_mask, sign = masks(slot)
            north, southern = [], []
            for i in range(4):
                if members[i] == number:
                    parts = jnp.concatenate([tiles[i] * even_mask, tiles[i] * odd_mask], 0)
                    north.append(parts)
                    southern.append(parts * sign)
                    here = (lane // 32 == i) & (lane % 32 < 16)
                    zero = zero + jnp.where(p == 0, 1.0, 0.0) * here.astype(jnp.float32)
                else:
                    north.append(empty)
                    southern.append(empty)
            right_high, right_low = split(jnp.concatenate(north + southern, 0))
            high = table_high[slot]
            product = (
                dot_nt(high, right_high) + dot_nt(high, right_low) + dot_nt(table_low[slot], right_high)
            )
            result = product if result is None else result + product
        for lat in range(10):
            rows = result[lat * 32 : (lat + 1) * 32]
            target[pl.ds(first_row + lat, 32, stride=stride), :] = rows[:, 0:128]
            target[pl.ds(first_row + lat + 32 * stride, 32, stride=stride), :] = rows[:, 128:256]
        squares = result * result
        squares = squares[:, 0:128] + squares[:, 128:256]
        total = jnp.sum(squares.reshape(40, 8, 128), axis=0)
        real = 1.0 - ((lane // 8) % 2).astype(jnp.float32)
        total = total * (2.0 * (1.0 - zero) + real * zero)
        for i in range(4):
            energy[groups[i]] = energy[groups[i]] + total * (lane // 32 == i).astype(jnp.float32)

    def wave_copy(chunk, i):
        dest = partner(i)
        size = ROWS if chunk < 3 else LAST
        source = waves_send.at[chunk] if chunk < 3 else last_send
        sink = waves.at[chunk] if chunk < 3 else last
        return pltpu.make_async_remote_copy(
            src_ref=source.at[pl.ds(pl.multiple_of(block_of(dest) * size, 8), size)],
            dst_ref=sink.at[pl.ds(pl.multiple_of(wide * size, 8), size)],
            send_sem=waves_send_sem.at[chunk],
            recv_sem=waves_sem.at[chunk],
            device_id={"grp": grp, "wide": dest},
            device_id_type=MESH,
        )

    def wave_all(chunk):
        size = ROWS if chunk < 3 else LAST
        source = waves_send.at[chunk] if chunk < 3 else last_send
        sink = waves.at[chunk] if chunk < 3 else last
        return pltpu.make_async_remote_copy(
            src_ref=source.at[pl.ds(0, (PEERS - 1) * size)],
            dst_ref=sink.at[pl.ds(0, (PEERS - 1) * size)],
            send_sem=waves_send_sem.at[chunk],
            recv_sem=waves_sem.at[chunk],
            device_id={"grp": grp, "wide": partner(0)},
            device_id_type=MESH,
        )

    def send_waves(chunk):
        def one(i, carry):
            wave_copy(chunk, i).start()
            return carry

        lax.fori_loop(0, PEERS - 1, one, 0)
        size = ROWS if chunk < 3 else LAST
        source = waves_send.at[chunk] if chunk < 3 else last_send
        sink = waves.at[chunk] if chunk < 3 else last
        sink[pl.ds(pl.multiple_of(wide * size, 8), size), :] = source[
            pl.ds(pl.multiple_of(block_of(wide) * size, 8), size), :
        ]

    def own_row(r, carry):
        wave_row(
            (r, 4),
            (0, 0, 0, 1),
            [piece(None, q, r) for q in range(3)] + [piece(None, r, 4)],
            (0, 1, 2, r),
            last_send,
            r * 10,
            LAST,
        )
        return carry

    lax.fori_loop(0, 2, own_row, 0)
    wave_row(
        (2, 3),
        (0, 0, 1, 1),
        [piece(None, 0, 2), piece(None, 1, 2), piece(None, 0, 3), piece(None, 1, 3)],
        (0, 1, 0, 1),
        last_send,
        20,
        LAST,
    )
    spare = jnp.zeros((64, 128), jnp.float32)
    last_send[pl.ds(30, 64, stride=LAST), :] = spare
    last_send[pl.ds(31, 64, stride=LAST), :] = spare

    pl.semaphore_wait(barrier, PEERS - 1 + GROUPS - 1)
    send_waves(3)
    lax.fori_loop(5, 20, reorder, 0)
    for chunk in range(3):
        for step in (1, 2, 3):
            coeffs_copy(chunk, step).start()

    def waves_of(q):
        coeffs_all(q).wait_recv()
        e, f, h = (4, 3, 3) if q == 0 else (4, 3, 2) if q == 1 else (3, 4, 4)

        def one(r, carry):
            wave_row(
                (r, e),
                (0, 0, 0, 1),
                [piece(dx, q, r) for dx in (1, 2, 3)] + [piece(r + 1, q, e)],
                (3 + q, 6 + q, 9 + q, 3 * (r + 1) + q),
                waves_send.at[q],
                r * 10,
                ROWS,
            )
            return carry

        lax.fori_loop(0, 3, one, 0)
        wave_row(
            (f,) if f == h else (f, h),
            (0, 0, 0, 0) if f == h else (0, 0, 0, 1),
            [piece(dx, q, f) for dx in (1, 2, 3)] + [piece(None, 2, h)],
            (3 + q, 6 + q, 9 + q, 2),
            waves_send.at[q],
            30,
            ROWS,
        )

    waves_of(0)
    send_waves(0)
    waves_of(1)
    send_waves(1)
    waves_of(2)

    share = jnp.zeros((1, 128), jnp.float32)
    for group in range(12):
        row = jnp.sum(energy[group], axis=0, keepdims=True)
        for shift in (64, 32, 16, 8):
            row = row + pltpu.roll(row, shift, 1)
        share = jnp.where(lane // 8 == group, row, share)
    shares_send[0] = share
    shares[wide] = share

    def share_copy(i):
        return pltpu.make_async_remote_copy(
            src_ref=shares_send.at[0],
            dst_ref=shares.at[wide],
            send_sem=shares_send_sem,
            recv_sem=shares_sem,
            device_id={"grp": grp, "wide": partner(i)},
            device_id_type=MESH,
        )

    def send_share(i, carry):
        share_copy(i).start()
        return carry

    lax.fori_loop(0, PEERS - 1, send_share, 0)
    send_waves(2)

    def cosine(phase):
        phase = phase - LON * jnp.floor(phase * (1.0 / LON) + 0.5)
        angle = (LON // 4 - jnp.abs(phase)) * (2.0 * math.pi / LON)
        square = angle * angle
        series = 1.0 / 6227020800.0
        for term in (-1.0 / 39916800.0, 1.0 / 362880.0, -1.0 / 5040.0, 1.0 / 120.0, -1.0 / 6.0, 1.0):
            series = series * square + term
        return series * angle

    column = lax.broadcasted_iota(jnp.int32, (64, 128), 1)

    def spread_pairs(i, carry):
        for slot in range(5):
            pairs_down[pl.ds(slot * 64 + i, 1), :] = jnp.full((1, 128), pair[i * 5 + slot])
        return carry

    lax.fori_loop(0, PEERS, spread_pairs, 0)

    def make_synthesis(i, carry):
        parity, slot = i // 5, i % 5
        p = pairs_down[pl.ds(pl.multiple_of(slot * 64, 64), 64), :]
        number = jnp.where(p % 2 == parity, p, WAVES - 1 - p)
        factor = jnp.where(number == 0, 1.0, 2.0)
        cos_row = pl.multiple_of(slot * 64 + (slot // 4) * 256, 64)
        sin_row = pl.multiple_of(256 + slot * 64 + (slot // 4) * 64, 64)
        for tile in range(5):
            phase = (number * (column + tile * 128)).astype(jnp.float32)
            lanes = pl.ds(tile * 128, 128)
            high, low = split(factor * cosine(phase))
            synth_high[parity, pl.ds(cos_row, 64), lanes] = high
            synth_low[parity, pl.ds(cos_row, 64), lanes] = low
            high, low = split(-factor * cosine(phase - LON // 4))
            synth_high[parity, pl.ds(sin_row, 64), lanes] = high
            synth_low[parity, pl.ds(sin_row, 64), lanes] = low
        return carry

    lax.fori_loop(0, 10, make_synthesis, 0)

    def place_of(q, dx, slot):
        if dx == 0 and q < 2:
            return {0: (3, 0, q), 1: (3, 1, q), 2: (3, 2, q), 3: (3, 2, 2 + q), 4: (3, q, 3)}[slot]
        if dx == 0:
            return {0: (3, 0, 2), 1: (3, 1, 2), 2: (1, 3, 3), 3: (0, 3, 3), 4: (2, 3, 3)}[slot]
        e, f = (4, 3) if q < 2 else (3, 4)
        if slot == e:
            return (q, dx - 1, 3)
        return (q, 3 if slot == f else slot, dx - 1)

    def synthesis(q):
        def turn(lat, carry):
            turned = {}
            for dx in range(GROUPS):
                group = lax.rem(grp + dx, GROUPS)
                rows = pl.ds(pl.multiple_of(lat * 32 + group * 8, 8), 8)
                for slot in range(5):
                    message, row, place = place_of(q, dx, slot)
                    if (message, row) not in turned:
                        if message < 3:
                            value = waves[message, pl.ds(row * 10 + lat, 64, stride=ROWS), :]
                        else:
                            value = last[pl.ds(row * 10 + lat, 64, stride=LAST), :]
                        turned[message, row] = value.T
                    for parity in range(2):
                        for c in range(2):
                            at = place * 32 + parity * 16 + c * 8
                            column = c * 256 + slot * 64 if slot < 4 else 512 + c * 64
                            left[parity, rows, column : column + 64] = turned[message, row][
                                at : at + 8
                            ]
            return carry

        lax.fori_loop(0, 10, turn, 0)

        def part(i, carry):
            rows = pl.ds(pl.multiple_of(i * 32, 32), 32)
            for parity in range(2):
                high, low = split(left[parity, rows, :])
                left_high[parity, rows, :] = high
                left_low[parity, rows, :] = low
            return carry

        lax.fori_loop(0, 10, part, 0)

        def dot(a, b):
            return jnp.dot(a, b, preferred_element_type=jnp.float32)

        for start, width in ((0, 256), (256, 256), (512, 128)):
            halves = []
            for parity in range(2):
                right_high = synth_high[parity, :, start : start + width]
                right_low = synth_low[parity, :, start : start + width]
                halves.append(
                    dot(left_high[parity], right_high)
                    + dot(left_high[parity], right_low)
                    + dot(left_low[parity], right_high)
                )
            for value, offset in ((halves[0] + halves[1], 0), (halves[0] - halves[1], HALF)):
                for lat in range(10):
                    place = lat + south * (9 - 2 * lat)
                    for g in range(GROUPS):
                        for j in range(2):
                            row = lat * 32 + g * 8 + j * 4
                            level = g * 12 + q * 4
                            out[
                                j,
                                place,
                                level : level + 4,
                                offset + start : offset + start + width,
                            ] = value[row : row + 4]

    wave_all(3).wait_recv()
    wave_all(0).wait_recv()

    def sums_copy(step):
        dest = other_group(step)
        return pltpu.make_async_remote_copy(
            src_ref=sums.at[grp],
            dst_ref=sums.at[grp],
            send_sem=sums_send_sem,
            recv_sem=sums_sem,
            device_id={"grp": dest, "wide": wide},
            device_id_type=MESH,
        )

    synthesis(0)
    wave_all(1).wait_recv()
    synthesis(1)

    shares_all = pltpu.make_async_remote_copy(
        src_ref=shares.at[pl.ds(0, PEERS - 1)],
        dst_ref=shares.at[pl.ds(0, PEERS - 1)],
        send_sem=shares_send_sem,
        recv_sem=shares_sem,
        device_id={"grp": grp, "wide": partner(0)},
        device_id_type=MESH,
    )
    shares_all.wait_send()
    shares_all.wait_recv()
    sums[grp] = jnp.broadcast_to(jnp.sum(shares[...], axis=0), (8, 128))
    for step in (1, 2, 3):
        sums_copy(step).start()
    sums_all = pltpu.make_async_remote_copy(
        src_ref=sums.at[0:3],
        dst_ref=sums.at[0:3],
        send_sem=sums_send_sem,
        recv_sem=sums_sem,
        device_id={"grp": other_group(1), "wide": wide},
        device_id_type=MESH,
    )
    sums_all.wait_send()
    sums_all.wait_recv()
    sums_out[...] = sums[...]
    wave_all(2).wait_recv()
    synthesis(2)
    for chunk in range(3):
        coeffs_all(chunk).wait_send()
    for chunk in range(4):
        wave_all(chunk).wait_send()


def local(spectral, legendre, pair_table, field_map):
    table = jnp.swapaxes(legendre, 1, 2)
    smem = pl.BlockSpec(memory_space=pltpu.SMEM)
    vmem = pl.BlockSpec(memory_space=pltpu.VMEM)
    dma = pltpu.SemaphoreType.DMA
    grid, sums = pl.pallas_call(
        kernel,
        name="transform",
        out_shape=(
            jax.ShapeDtypeStruct((2, 10, 48, LON), jnp.float32),
            jax.ShapeDtypeStruct((GROUPS, 8, 128), jnp.float32),
        ),
        in_specs=[smem, smem, vmem, pl.BlockSpec(memory_space=pltpu.HBM)],
        out_specs=(vmem, vmem),
        scratch_shapes=[
            pltpu.VMEM((5, 320, 641), jnp.float32),
            pltpu.VMEM((6, 5, 320, 128), jnp.float32),
            pltpu.VMEM((320, 128), jnp.int32),
            pltpu.VMEM((5, 320, 768), jnp.bfloat16),
            pltpu.VMEM((5, 320, 768), jnp.bfloat16),
            pltpu.VMEM((GROUPS, 15, 16, 768), jnp.float32),
            pltpu.VMEM((GROUPS, 15, 16, 768), jnp.float32),
            pltpu.VMEM((3, PEERS * ROWS, 128), jnp.float32),
            pltpu.VMEM((PEERS * LAST, 128), jnp.float32),
            pltpu.VMEM((3, PEERS * ROWS, 128), jnp.float32),
            pltpu.VMEM((PEERS * LAST, 128), jnp.float32),
            pltpu.VMEM((2, HALF, HALF), jnp.bfloat16),
            pltpu.VMEM((2, HALF, HALF), jnp.bfloat16),
            pltpu.VMEM((2, 320, HALF), jnp.bfloat16),
            pltpu.VMEM((2, 320, HALF), jnp.bfloat16),
            pltpu.VMEM((2, 320, HALF), jnp.float32),
            pltpu.VMEM((12, 8, 128), jnp.float32),
            pltpu.VMEM((1, 1, 128), jnp.float32),
            pltpu.VMEM((PEERS, 1, 128), jnp.float32),
            pltpu.VMEM((GROUPS, 8, 128), jnp.float32),
            dma((6,)),
            dma((3,)),
            dma((3,)),
            dma((4,)),
            dma((4,)),
            dma,
            dma,
            dma,
            dma,
        ],
        compiler_params=pltpu.CompilerParams(
            collective_id=0, has_side_effects=True, vmem_limit_bytes=58 * 2**20
        ),
    )(pair_table, field_map, spectral, table)
    grid = jnp.swapaxes(grid, 1, 2)
    by_step = sums[:, 0, 0:96].reshape(GROUPS, GROUPS, 3, 2, 4)
    by_group = jnp.stack([jnp.roll(by_step[group], group, 0) for group in range(GROUPS)])
    checksums = jnp.transpose(by_group, (0, 3, 1, 2, 4)).reshape(8, 48) * (1.0 / LAT)
    return grid, checksums


def solution(mesh):
    placed = (P(None, "grp", "wide", None, None), P("wide", None, None), P(), P())
    return jax.shard_map(
        local,
        mesh=mesh,
        in_specs=placed,
        out_specs=(P("grp", None, "wide", None), P()),
        check_vma=False,
    )
```

```python
import functools
import math

import jax
import jax.numpy as jnp
from jax import lax
from jax.experimental import pallas as pl
from jax.experimental.pallas import tpu as pltpu
from jax.sharding import PartitionSpec as P

WAVES = 640
LAT = 640
LON = 1280
HALF = LON // 2
MESH = pl.DeviceIdType.MESH
ROWS = 40
LAST = 32
GROUPS = 4
PEERS = 64


def split(value):
    high = value.astype(jnp.bfloat16)
    low = (value - high.astype(jnp.float32)).astype(jnp.bfloat16)
    return high, low


def kernel(
    pair,
    fields,
    spectral,
    table_hbm,
    out,
    sums_out,
    table_whole,
    table,
    pairs_down,
    table_high,
    table_low,
    coeffs_send,
    coeffs,
    waves_send,
    last_send,
    waves,
    last,
    synth_high,
    synth_low,
    left_high,
    left_low,
    left,
    grid,
    energy,
    shares_send,
    shares,
    sums,
    table_sem,
    coeffs_send_sem,
    coeffs_sem,
    waves_send_sem,
    waves_sem,
    shares_send_sem,
    shares_sem,
    sums_send_sem,
    sums_sem,
    out_sem,
):
    grp = lax.axis_index("grp")
    wide = lax.axis_index("wide")
    my_y, my_z, my_c = wide // 16, (wide // 2) % 8, wide % 2
    south = wide // 32

    def other_group(step):
        return lax.rem(grp + step, GROUPS)

    def partner(i):
        k = i % 8
        up = (k + 2) // 2
        dz = (k % 2) * (8 - up) + (1 - k % 2) * up
        dz = (1 - k // 6) * dz + (k // 6) * (1 - k % 2) * 4
        dy = 3 - (i // 8) % 4
        dc = 1 - i // 32
        return (
            lax.rem(my_y + dy, 4) * 16 + lax.rem(my_z + dz, 8) * 2 + lax.rem(my_c + dc, 2)
        )

    def block_of(dest):
        return dest + (dest // 32) * (95 - 2 * dest)

    barrier = pltpu.get_barrier_semaphore()
    table_copies = [
        pltpu.make_async_copy(
            table_hbm.at[:, :, tile * 128 : (tile + 1) * 128],
            table.at[tile],
            table_sem.at[tile],
        )
        for tile in range(5)
    ] + [pltpu.make_async_copy(table_hbm, table_whole, table_sem.at[5])]
    for copy in table_copies:
        copy.start()

    def greet(i, carry):
        pl.semaphore_signal(
            barrier, inc=1, device_id={"grp": grp, "wide": partner(i)}, device_id_type=MESH
        )
        return carry

    lax.fori_loop(0, PEERS - 1, greet, 0)
    for step in (1, 2, 3):
        pl.semaphore_signal(
            barrier,
            inc=1,
            device_id={"grp": other_group(step), "wide": wide},
            device_id_type=MESH,
        )

    coeffs_send[:, :, :, 640:768] = jnp.zeros((GROUPS, 15, 16, 128), jnp.float32)

    def reorder(i, carry):
        group, slot = lax.rem(grp + i // 5, GROUPS), i % 5
        for j in range(2):
            field = fields[2 * group + j]
            for level in range(12):
                q, l = level // 4, level % 4
                for c in range(2):
                    coeffs_send[group, q * 5 + slot, c * 8 + j * 4 + l, 0:641] = spectral[
                        field, level, slot, c, :
                    ]
        return carry

    lax.fori_loop(0, 5, reorder, 0)

    def coeffs_copy(chunk, step):
        blocks = pl.ds(chunk * 5, 5)
        dest = other_group(step)
        return pltpu.make_async_remote_copy(
            src_ref=coeffs_send.at[dest, blocks],
            dst_ref=coeffs.at[grp, blocks],
            send_sem=coeffs_send_sem.at[chunk],
            recv_sem=coeffs_sem.at[chunk],
            device_id={"grp": dest, "wide": wide},
            device_id_type=MESH,
        )

    def coeffs_all(chunk):
        blocks = pl.ds(chunk * 5, 5)
        return pltpu.make_async_remote_copy(
            src_ref=coeffs_send.at[0:3, blocks],
            dst_ref=coeffs.at[0:3, blocks],
            send_sem=coeffs_send_sem.at[chunk],
            recv_sem=coeffs_sem.at[chunk],
            device_id={"grp": other_group(1), "wide": wide},
            device_id_type=MESH,
        )

    for copy in table_copies:
        copy.wait()
    first_lane = lax.broadcasted_iota(jnp.int32, (320, 128), 1) == 0

    def part_end(slot, carry):
        table[5, slot] = jnp.where(first_lane, table_whole[slot, :, 640:641], 0.0)
        return carry

    lax.fori_loop(0, 5, part_end, 0)

    def part_table(i, carry):
        slot, lat = i // 10, i % 10
        rows = pl.ds(pl.multiple_of(lat * 32, 32), 32)
        for tile in range(6):
            value = table[tile, slot, pl.ds(lat, 32, stride=10), :]
            high, low = split(value)
            table_high[slot, rows, tile * 128 : (tile + 1) * 128] = high
            table_low[slot, rows, tile * 128 : (tile + 1) * 128] = low
        return carry

    lax.fori_loop(0, 50, part_table, 0)

    energy[...] = jnp.zeros_like(energy)
    degree = lax.broadcasted_iota(jnp.int32, (1, 768), 1)
    lane = lax.broadcasted_iota(jnp.int32, (1, 128), 1)

    def masks(slot):
        p = pair[wide * 5 + slot]
        boundary = WAVES - p
        first_part = degree < boundary
        start = jnp.where(first_part, 0, boundary)
        sign = 1.0 - 2.0 * ((degree - start) % 2).astype(jnp.float32)
        is_first = first_part.astype(jnp.float32)
        inside = (degree <= WAVES).astype(jnp.float32)
        odd = (p % 2).astype(jnp.float32)
        even_mask = (is_first * (1.0 - odd) + (1.0 - is_first) * odd) * inside
        odd_mask = (1.0 - even_mask) * inside
        return p, even_mask, odd_mask, sign

    def piece(dx, q, slot):
        if dx is None:
            return coeffs_send[grp, q * 5 + slot]
        return coeffs[lax.rem(grp + dx, GROUPS), q * 5 + slot]

    nt = (((1,), (1,)), ((), ()))

    def dot_nt(a, b):
        return lax.dot_general(a, b, nt, preferred_element_type=jnp.float32)

    def wave_row(slots, members, tiles, groups, target, first_row, stride):
        result = None
        zero = jnp.zeros((1, 128), jnp.float32)
        empty = jnp.zeros((32, 768), jnp.float32)
        for number, slot in enumerate(slots):
            p, even_mask, odd_mask, sign = masks(slot)
            north, southern = [], []
            for i in range(4):
                if members[i] == number:
                    parts = jnp.concatenate([tiles[i] * even_mask, tiles[i] * odd_mask], 0)
                    north.append(parts)
                    southern.append(parts * sign)
                    here = (lane // 32 == i) & (lane % 32 < 16)
                    zero = zero + jnp.where(p == 0, 1.0, 0.0) * here.astype(jnp.float32)
                else:
                    north.append(empty)
                    southern.append(empty)
            right_high, right_low = split(jnp.concatenate(north + southern, 0))
            high = table_high[slot]
            product = (
                dot_nt(high, right_high) + dot_nt(high, right_low) + dot_nt(table_low[slot], right_high)
            )
            result = product if result is None else result + product
        for lat in range(10):
            rows = result[lat * 32 : (lat + 1) * 32]
            target[pl.ds(first_row + lat, 32, stride=stride), :] = rows[:, 0:128]
            target[pl.ds(first_row + lat + 32 * stride, 32, stride=stride), :] = rows[:, 128:256]
        squares = result * result
        squares = squares[:, 0:128] + squares[:, 128:256]
        total = jnp.sum(squares.reshape(40, 8, 128), axis=0)
        real = 1.0 - ((lane // 8) % 2).astype(jnp.float32)
        total = total * (2.0 * (1.0 - zero) + real * zero)
        for i in range(4):
            energy[groups[i]] = energy[groups[i]] + total * (lane // 32 == i).astype(jnp.float32)

    def wave_copy(chunk, i):
        dest = partner(i)
        size = ROWS if chunk < 3 else LAST
        source = waves_send.at[chunk] if chunk < 3 else last_send
        sink = waves.at[chunk] if chunk < 3 else last
        return pltpu.make_async_remote_copy(
            src_ref=source.at[pl.ds(pl.multiple_of(block_of(dest) * size, 8), size)],
            dst_ref=sink.at[pl.ds(pl.multiple_of(wide * size, 8), size)],
            send_sem=waves_send_sem.at[chunk],
            recv_sem=waves_sem.at[chunk],
            device_id={"grp": grp, "wide": dest},
            device_id_type=MESH,
        )

    def wave_all(chunk):
        size = ROWS if chunk < 3 else LAST
        source = waves_send.at[chunk] if chunk < 3 else last_send
        sink = waves.at[chunk] if chunk < 3 else last
        return pltpu.make_async_remote_copy(
            src_ref=source.at[pl.ds(0, (PEERS - 1) * size)],
            dst_ref=sink.at[pl.ds(0, (PEERS - 1) * size)],
            send_sem=waves_send_sem.at[chunk],
            recv_sem=waves_sem.at[chunk],
            device_id={"grp": grp, "wide": partner(0)},
            device_id_type=MESH,
        )

    def send_waves(chunk):
        def one(i, carry):
            wave_copy(chunk, i).start()
            return carry

        lax.fori_loop(0, PEERS - 1, one, 0)
        size = ROWS if chunk < 3 else LAST
        source = waves_send.at[chunk] if chunk < 3 else last_send
        sink = waves.at[chunk] if chunk < 3 else last
        sink[pl.ds(pl.multiple_of(wide * size, 8), size), :] = source[
            pl.ds(pl.multiple_of(block_of(wide) * size, 8), size), :
        ]

    def own_row(r, carry):
        wave_row(
            (r, 4),
            (0, 0, 0, 1),
            [piece(None, q, r) for q in range(3)] + [piece(None, r, 4)],
            (0, 1, 2, r),
            last_send,
            r * 10,
            LAST,
        )
        return carry

    lax.fori_loop(0, 2, own_row, 0)
    wave_row(
        (2, 3),
        (0, 0, 1, 1),
        [piece(None, 0, 2), piece(None, 1, 2), piece(None, 0, 3), piece(None, 1, 3)],
        (0, 1, 0, 1),
        last_send,
        20,
        LAST,
    )
    spare = jnp.zeros((64, 128), jnp.float32)
    last_send[pl.ds(30, 64, stride=LAST), :] = spare
    last_send[pl.ds(31, 64, stride=LAST), :] = spare

    pl.semaphore_wait(barrier, PEERS - 1 + GROUPS - 1)
    send_waves(3)
    lax.fori_loop(5, 20, reorder, 0)
    for chunk in range(3):
        for step in (1, 2, 3):
            coeffs_copy(chunk, step).start()

    def waves_of(q):
        coeffs_all(q).wait_recv()
        e, f, h = (4, 3, 3) if q == 0 else (4, 3, 2) if q == 1 else (3, 4, 4)

        def one(r, carry):
            wave_row(
                (r, e),
                (0, 0, 0, 1),
                [piece(dx, q, r) for dx in (1, 2, 3)] + [piece(r + 1, q, e)],
                (3 + q, 6 + q, 9 + q, 3 * (r + 1) + q),
                waves_send.at[q],
                r * 10,
                ROWS,
            )
            return carry

        lax.fori_loop(0, 3, one, 0)
        wave_row(
            (f,) if f == h else (f, h),
            (0, 0, 0, 0) if f == h else (0, 0, 0, 1),
            [piece(dx, q, f) for dx in (1, 2, 3)] + [piece(None, 2, h)],
            (3 + q, 6 + q, 9 + q, 2),
            waves_send.at[q],
            30,
            ROWS,
        )

    waves_of(0)
    send_waves(0)
    waves_of(1)
    send_waves(1)
    waves_of(2)

    share = jnp.zeros((1, 128), jnp.float32)
    for group in range(12):
        row = jnp.sum(energy[group], axis=0, keepdims=True)
        for shift in (64, 32, 16, 8):
            row = row + pltpu.roll(row, shift, 1)
        share = jnp.where(lane // 8 == group, row, share)
    shares_send[0] = share
    shares[wide] = share

    def share_copy(i):
        return pltpu.make_async_remote_copy(
            src_ref=shares_send.at[0],
            dst_ref=shares.at[wide],
            send_sem=shares_send_sem,
            recv_sem=shares_sem,
            device_id={"grp": grp, "wide": partner(i)},
            device_id_type=MESH,
        )

    def send_share(i, carry):
        share_copy(i).start()
        return carry

    lax.fori_loop(0, PEERS - 1, send_share, 0)
    send_waves(2)

    def cosine(phase):
        phase = phase - LON * jnp.floor(phase * (1.0 / LON) + 0.5)
        angle = (LON // 4 - jnp.abs(phase)) * (2.0 * math.pi / LON)
        square = angle * angle
        series = 1.0 / 6227020800.0
        for term in (-1.0 / 39916800.0, 1.0 / 362880.0, -1.0 / 5040.0, 1.0 / 120.0, -1.0 / 6.0, 1.0):
            series = series * square + term
        return series * angle

    column = lax.broadcasted_iota(jnp.int32, (64, 128), 1)

    def spread_pairs(i, carry):
        for slot in range(5):
            pairs_down[pl.ds(slot * 64 + i, 1), :] = jnp.full((1, 128), pair[i * 5 + slot])
        return carry

    lax.fori_loop(0, PEERS, spread_pairs, 0)

    def make_synthesis(i, carry):
        parity, slot = i // 5, i % 5
        p = pairs_down[pl.ds(pl.multiple_of(slot * 64, 64), 64), :]
        number = jnp.where(p % 2 == parity, p, WAVES - 1 - p)
        factor = jnp.where(number == 0, 1.0, 2.0)
        cos_row = pl.multiple_of(slot * 64 + (slot // 4) * 256, 64)
        sin_row = pl.multiple_of(256 + slot * 64 + (slot // 4) * 64, 64)
        for tile in range(5):
            phase = (number * (column + tile * 128)).astype(jnp.float32)
            lanes = pl.ds(tile * 128, 128)
            high, low = split(factor * cosine(phase))
            synth_high[parity, pl.ds(cos_row, 64), lanes] = high
            synth_low[parity, pl.ds(cos_row, 64), lanes] = low
            high, low = split(-factor * cosine(phase - LON // 4))
            synth_high[parity, pl.ds(sin_row, 64), lanes] = high
            synth_low[parity, pl.ds(sin_row, 64), lanes] = low
        return carry

    lax.fori_loop(0, 10, make_synthesis, 0)

    def out_copy(first, width):
        columns = pl.ds(first, width)
        return pltpu.make_async_copy(
            grid.at[:, :, :, columns], out.at[:, :, :, columns], out_sem.at[first // 128]
        )

    def place_of(q, dx, slot):
        if dx == 0 and q < 2:
            return {0: (3, 0, q), 1: (3, 1, q), 2: (3, 2, q), 3: (3, 2, 2 + q), 4: (3, q, 3)}[slot]
        if dx == 0:
            return {0: (3, 0, 2), 1: (3, 1, 2), 2: (1, 3, 3), 3: (0, 3, 3), 4: (2, 3, 3)}[slot]
        e, f = (4, 3) if q < 2 else (3, 4)
        if slot == e:
            return (q, dx - 1, 3)
        return (q, 3 if slot == f else slot, dx - 1)

    def gather(q, messages):
        def turn(lat, carry):
            turned = {}
            for dx in range(GROUPS):
                group = lax.rem(grp + dx, GROUPS)
                rows = pl.ds(pl.multiple_of(lat * 32 + group * 8, 8), 8)
                for slot in range(5):
                    message, row, place = place_of(q, dx, slot)
                    if message not in messages:
                        continue
                    if (message, row) not in turned:
                        if message < 3:
                            value = waves[message, pl.ds(row * 10 + lat, 64, stride=ROWS), :]
                        else:
                            value = last[pl.ds(row * 10 + lat, 64, stride=LAST), :]
                        turned[message, row] = value.T
                    for parity in range(2):
                        for c in range(2):
                            at = place * 32 + parity * 16 + c * 8
                            column = c * 256 + slot * 64 if slot < 4 else 512 + c * 64
                            left[parity, rows, column : column + 64] = turned[message, row][
                                at : at + 8
                            ]
            return carry

        lax.fori_loop(0, 10, turn, 0)

    def synthesis(q):
        def part(i, carry):
            rows = pl.ds(pl.multiple_of(i * 32, 32), 32)
            for parity in range(2):
                high, low = split(left[parity, rows, :])
                left_high[parity, rows, :] = high
                left_low[parity, rows, :] = low
            return carry

        lax.fori_loop(0, 10, part, 0)

        def dot(a, b):
            return jnp.dot(a, b, preferred_element_type=jnp.float32)

        for start, width in ((0, 256), (256, 256), (512, 128)):
            halves = []
            for parity in range(2):
                right_high = synth_high[parity, :, start : start + width]
                right_low = synth_low[parity, :, start : start + width]
                halves.append(
                    dot(left_high[parity], right_high)
                    + dot(left_high[parity], right_low)
                    + dot(left_low[parity], right_high)
                )
            for value, offset in ((halves[0] + halves[1], 0), (halves[0] - halves[1], HALF)):
                for lat in range(10):
                    place = lat + south * (9 - 2 * lat)
                    for g in range(GROUPS):
                        for j in range(2):
                            row = lat * 32 + g * 8 + j * 4
                            level = g * 12 + q * 4
                            grid[
                                j,
                                place,
                                level : level + 4,
                                offset + start : offset + start + width,
                            ] = value[row : row + 4]
                if q == 2:
                    out_copy(offset + start, width).start()

    wave_all(3).wait_recv()
    wave_all(0).wait_recv()

    def sums_copy(step):
        dest = other_group(step)
        return pltpu.make_async_remote_copy(
            src_ref=sums.at[grp],
            dst_ref=sums.at[grp],
            send_sem=sums_send_sem,
            recv_sem=sums_sem,
            device_id={"grp": dest, "wide": wide},
            device_id_type=MESH,
        )

    gather(0, (3, 0))
    synthesis(0)
    wave_all(1).wait_recv()
    gather(1, (3, 1))
    synthesis(1)
    gather(2, (3, 0, 1))

    shares_all = pltpu.make_async_remote_copy(
        src_ref=shares.at[pl.ds(0, PEERS - 1)],
        dst_ref=shares.at[pl.ds(0, PEERS - 1)],
        send_sem=shares_send_sem,
        recv_sem=shares_sem,
        device_id={"grp": grp, "wide": partner(0)},
        device_id_type=MESH,
    )
    shares_all.wait_send()
    shares_all.wait_recv()
    sums[grp] = jnp.broadcast_to(jnp.sum(shares[...], axis=0), (8, 128))
    for step in (1, 2, 3):
        sums_copy(step).start()
    sums_all = pltpu.make_async_remote_copy(
        src_ref=sums.at[0:3],
        dst_ref=sums.at[0:3],
        send_sem=sums_send_sem,
        recv_sem=sums_sem,
        device_id={"grp": other_group(1), "wide": wide},
        device_id_type=MESH,
    )
    sums_all.wait_send()
    sums_all.wait_recv()
    sums_out[...] = sums[...]
    wave_all(2).wait_recv()
    gather(2, (2,))
    synthesis(2)
    for chunk in range(3):
        coeffs_all(chunk).wait_send()
    for chunk in range(4):
        wave_all(chunk).wait_send()
    for start, width in ((0, 256), (256, 256), (512, 128)):
        for offset in (0, HALF):
            out_copy(offset + start, width).wait()


def local(spectral, legendre, pair_table, field_map):
    table = jnp.swapaxes(legendre, 1, 2)
    smem = pl.BlockSpec(memory_space=pltpu.SMEM)
    vmem = pl.BlockSpec(memory_space=pltpu.VMEM)
    dma = pltpu.SemaphoreType.DMA
    grid, sums = pl.pallas_call(
        kernel,
        name="transform",
        out_shape=(
            jax.ShapeDtypeStruct((2, 10, 48, LON), jnp.float32),
            jax.ShapeDtypeStruct((GROUPS, 8, 128), jnp.float32),
        ),
        in_specs=[smem, smem, vmem, pl.BlockSpec(memory_space=pltpu.HBM)],
        out_specs=(pl.BlockSpec(memory_space=pltpu.HBM), vmem),
        scratch_shapes=[
            pltpu.VMEM((5, 320, 641), jnp.float32),
            pltpu.VMEM((6, 5, 320, 128), jnp.float32),
            pltpu.VMEM((320, 128), jnp.int32),
            pltpu.VMEM((5, 320, 768), jnp.bfloat16),
            pltpu.VMEM((5, 320, 768), jnp.bfloat16),
            pltpu.VMEM((GROUPS, 15, 16, 768), jnp.float32),
            pltpu.VMEM((GROUPS, 15, 16, 768), jnp.float32),
            pltpu.VMEM((3, PEERS * ROWS, 128), jnp.float32),
            pltpu.VMEM((PEERS * LAST, 128), jnp.float32),
            pltpu.VMEM((3, PEERS * ROWS, 128), jnp.float32),
            pltpu.VMEM((PEERS * LAST, 128), jnp.float32),
            pltpu.VMEM((2, HALF, HALF), jnp.bfloat16),
            pltpu.VMEM((2, HALF, HALF), jnp.bfloat16),
            pltpu.VMEM((2, 320, HALF), jnp.bfloat16),
            pltpu.VMEM((2, 320, HALF), jnp.bfloat16),
            pltpu.VMEM((2, 320, HALF), jnp.float32),
            pltpu.VMEM((2, 10, 48, LON), jnp.float32),
            pltpu.VMEM((12, 8, 128), jnp.float32),
            pltpu.VMEM((1, 1, 128), jnp.float32),
            pltpu.VMEM((PEERS, 1, 128), jnp.float32),
            pltpu.VMEM((GROUPS, 8, 128), jnp.float32),
            dma((6,)),
            dma((3,)),
            dma((3,)),
            dma((4,)),
            dma((4,)),
            dma,
            dma,
            dma,
            dma,
            dma((10,)),
        ],
        compiler_params=pltpu.CompilerParams(
            collective_id=0, has_side_effects=True, vmem_limit_bytes=58 * 2**20
        ),
    )(pair_table, field_map, spectral, table)
    grid = jnp.swapaxes(grid, 1, 2)
    by_step = sums[:, 0, 0:96].reshape(GROUPS, GROUPS, 3, 2, 4)
    by_group = jnp.stack([jnp.roll(by_step[group], group, 0) for group in range(GROUPS)])
    checksums = jnp.transpose(by_group, (0, 3, 1, 2, 4)).reshape(8, 48) * (1.0 / LAT)
    return grid, checksums


def solution(mesh):
    placed = (P(None, "grp", "wide", None, None), P("wide", None, None), P(), P())
    return jax.shard_map(
        local,
        mesh=mesh,
        in_specs=placed,
        out_specs=(P("grp", None, "wide", None), P()),
        check_vma=False,
    )
```

```python
import functools
import math

import jax
import jax.numpy as jnp
from jax import lax
from jax.experimental import pallas as pl
from jax.experimental.pallas import tpu as pltpu
from jax.sharding import PartitionSpec as P

WAVES = 640
LAT = 640
LON = 1280
HALF = LON // 2
MESH = pl.DeviceIdType.MESH
ROWS = 40
LAST = 32
GROUPS = 4
PEERS = 64


def split(value):
    high = value.astype(jnp.bfloat16)
    low = (value - high.astype(jnp.float32)).astype(jnp.bfloat16)
    return high, low


def kernel(
    pair,
    fields,
    spectral,
    table_hbm,
    grid,
    sums_out,
    table_whole,
    table,
    pairs_down,
    table_high,
    table_low,
    coeffs_send,
    coeffs,
    waves_send,
    last_send,
    waves,
    last,
    synth_high,
    synth_low,
    left_high,
    left_low,
    left,
    energy,
    shares_send,
    shares,
    sums,
    table_sem,
    coeffs_send_sem,
    coeffs_sem,
    waves_send_sem,
    waves_sem,
    shares_send_sem,
    shares_sem,
    sums_send_sem,
    sums_sem,
):
    grp = lax.axis_index("grp")
    wide = lax.axis_index("wide")
    my_y, my_z, my_c = wide // 16, (wide // 2) % 8, wide % 2
    south = wide // 32

    def other_group(step):
        return lax.rem(grp + step, GROUPS)

    def partner(i):
        k = i % 8
        up = (k + 2) // 2
        dz = (k % 2) * (8 - up) + (1 - k % 2) * up
        dz = (1 - k // 6) * dz + (k // 6) * (1 - k % 2) * 4
        dy = 3 - (i // 8) % 4
        dc = 1 - i // 32
        return (
            lax.rem(my_y + dy, 4) * 16 + lax.rem(my_z + dz, 8) * 2 + lax.rem(my_c + dc, 2)
        )

    def block_of(dest):
        return dest + (dest // 32) * (95 - 2 * dest)

    barrier = pltpu.get_barrier_semaphore()
    table_copies = [
        pltpu.make_async_copy(
            table_hbm.at[:, :, tile * 128 : (tile + 1) * 128],
            table.at[tile],
            table_sem.at[tile],
        )
        for tile in range(5)
    ] + [pltpu.make_async_copy(table_hbm, table_whole, table_sem.at[5])]
    for copy in table_copies:
        copy.start()

    def greet(i, carry):
        pl.semaphore_signal(
            barrier, inc=1, device_id={"grp": grp, "wide": partner(i)}, device_id_type=MESH
        )
        return carry

    lax.fori_loop(0, PEERS - 1, greet, 0)
    for step in (1, 2, 3):
        pl.semaphore_signal(
            barrier,
            inc=1,
            device_id={"grp": other_group(step), "wide": wide},
            device_id_type=MESH,
        )

    coeffs_send[:, :, :, 640:768] = jnp.zeros((GROUPS, 15, 16, 128), jnp.float32)

    def reorder(i, carry):
        group, slot = lax.rem(grp + i // 5, GROUPS), i % 5
        for j in range(2):
            field = fields[2 * group + j]
            for level in range(12):
                q, l = level // 4, level % 4
                for c in range(2):
                    coeffs_send[group, q * 5 + slot, c * 8 + j * 4 + l, 0:641] = spectral[
                        field, level, slot, c, :
                    ]
        return carry

    lax.fori_loop(0, 5, reorder, 0)

    def coeffs_copy(chunk, step):
        blocks = pl.ds(chunk * 5, 5)
        dest = other_group(step)
        return pltpu.make_async_remote_copy(
            src_ref=coeffs_send.at[dest, blocks],
            dst_ref=coeffs.at[grp, blocks],
            send_sem=coeffs_send_sem.at[chunk],
            recv_sem=coeffs_sem.at[chunk],
            device_id={"grp": dest, "wide": wide},
            device_id_type=MESH,
        )

    def coeffs_all(chunk):
        blocks = pl.ds(chunk * 5, 5)
        return pltpu.make_async_remote_copy(
            src_ref=coeffs_send.at[0:3, blocks],
            dst_ref=coeffs.at[0:3, blocks],
            send_sem=coeffs_send_sem.at[chunk],
            recv_sem=coeffs_sem.at[chunk],
            device_id={"grp": other_group(1), "wide": wide},
            device_id_type=MESH,
        )

    for copy in table_copies:
        copy.wait()
    first_lane = lax.broadcasted_iota(jnp.int32, (320, 128), 1) == 0

    def part_end(slot, carry):
        table[5, slot] = jnp.where(first_lane, table_whole[slot, :, 640:641], 0.0)
        return carry

    lax.fori_loop(0, 5, part_end, 0)

    def part_table(i, carry):
        slot, lat = i // 10, i % 10
        rows = pl.ds(pl.multiple_of(lat * 32, 32), 32)
        for tile in range(6):
            value = table[tile, slot, pl.ds(lat, 32, stride=10), :]
            high, low = split(value)
            table_high[slot, rows, tile * 128 : (tile + 1) * 128] = high
            table_low[slot, rows, tile * 128 : (tile + 1) * 128] = low
        return carry

    lax.fori_loop(0, 50, part_table, 0)

    energy[...] = jnp.zeros_like(energy)
    degree = lax.broadcasted_iota(jnp.int32, (1, 768), 1)
    lane = lax.broadcasted_iota(jnp.int32, (1, 128), 1)

    def masks(slot):
        p = pair[wide * 5 + slot]
        boundary = WAVES - p
        first_part = degree < boundary
        start = jnp.where(first_part, 0, boundary)
        sign = 1.0 - 2.0 * ((degree - start) % 2).astype(jnp.float32)
        is_first = first_part.astype(jnp.float32)
        inside = (degree <= WAVES).astype(jnp.float32)
        odd = (p % 2).astype(jnp.float32)
        even_mask = (is_first * (1.0 - odd) + (1.0 - is_first) * odd) * inside
        odd_mask = (1.0 - even_mask) * inside
        return p, even_mask, odd_mask, sign

    def piece(dx, q, slot):
        if dx is None:
            return coeffs_send[grp, q * 5 + slot]
        return coeffs[lax.rem(grp + dx, GROUPS), q * 5 + slot]

    nt = (((1,), (1,)), ((), ()))

    def dot_nt(a, b):
        return lax.dot_general(a, b, nt, preferred_element_type=jnp.float32)

    def wave_row(slots, members, tiles, groups, target, first_row, stride):
        result = None
        zero = jnp.zeros((1, 128), jnp.float32)
        empty = jnp.zeros((32, 768), jnp.float32)
        for number, slot in enumerate(slots):
            p, even_mask, odd_mask, sign = masks(slot)
            north, southern = [], []
            for i in range(4):
                if members[i] == number:
                    parts = jnp.concatenate([tiles[i] * even_mask, tiles[i] * odd_mask], 0)
                    north.append(parts)
                    southern.append(parts * sign)
                    here = (lane // 32 == i) & (lane % 32 < 16)
                    zero = zero + jnp.where(p == 0, 1.0, 0.0) * here.astype(jnp.float32)
                else:
                    north.append(empty)
                    southern.append(empty)
            right_high, right_low = split(jnp.concatenate(north + southern, 0))
            high = table_high[slot]
            product = (
                dot_nt(high, right_high) + dot_nt(high, right_low) + dot_nt(table_low[slot], right_high)
            )
            result = product if result is None else result + product
        for lat in range(10):
            rows = result[lat * 32 : (lat + 1) * 32]
            target[pl.ds(first_row + lat, 32, stride=stride), :] = rows[:, 0:128]
            target[pl.ds(first_row + lat + 32 * stride, 32, stride=stride), :] = rows[:, 128:256]
        squares = result * result
        squares = squares[:, 0:128] + squares[:, 128:256]
        total = jnp.sum(squares.reshape(40, 8, 128), axis=0)
        real = 1.0 - ((lane // 8) % 2).astype(jnp.float32)
        total = total * (2.0 * (1.0 - zero) + real * zero)
        for i in range(4):
            energy[groups[i]] = energy[groups[i]] + total * (lane // 32 == i).astype(jnp.float32)

    def wave_copy(chunk, i):
        dest = partner(i)
        size = ROWS if chunk < 3 else LAST
        source = waves_send.at[chunk] if chunk < 3 else last_send
        sink = waves.at[chunk] if chunk < 3 else last
        return pltpu.make_async_remote_copy(
            src_ref=source.at[pl.ds(pl.multiple_of(block_of(dest) * size, 8), size)],
            dst_ref=sink.at[pl.ds(pl.multiple_of(wide * size, 8), size)],
            send_sem=waves_send_sem.at[chunk],
            recv_sem=waves_sem.at[chunk],
            device_id={"grp": grp, "wide": dest},
            device_id_type=MESH,
        )

    def wave_all(chunk):
        size = ROWS if chunk < 3 else LAST
        source = waves_send.at[chunk] if chunk < 3 else last_send
        sink = waves.at[chunk] if chunk < 3 else last
        return pltpu.make_async_remote_copy(
            src_ref=source.at[pl.ds(0, (PEERS - 1) * size)],
            dst_ref=sink.at[pl.ds(0, (PEERS - 1) * size)],
            send_sem=waves_send_sem.at[chunk],
            recv_sem=waves_sem.at[chunk],
            device_id={"grp": grp, "wide": partner(0)},
            device_id_type=MESH,
        )

    def send_waves(chunk):
        def one(i, carry):
            wave_copy(chunk, i).start()
            return carry

        lax.fori_loop(0, PEERS - 1, one, 0)
        size = ROWS if chunk < 3 else LAST
        source = waves_send.at[chunk] if chunk < 3 else last_send
        sink = waves.at[chunk] if chunk < 3 else last
        sink[pl.ds(pl.multiple_of(wide * size, 8), size), :] = source[
            pl.ds(pl.multiple_of(block_of(wide) * size, 8), size), :
        ]

    def own_row(r, carry):
        wave_row(
            (r, 4),
            (0, 0, 0, 1),
            [piece(None, q, r) for q in range(3)] + [piece(None, r, 4)],
            (0, 1, 2, r),
            last_send,
            r * 10,
            LAST,
        )
        return carry

    lax.fori_loop(0, 2, own_row, 0)
    wave_row(
        (2, 3),
        (0, 0, 1, 1),
        [piece(None, 0, 2), piece(None, 1, 2), piece(None, 0, 3), piece(None, 1, 3)],
        (0, 1, 0, 1),
        last_send,
        20,
        LAST,
    )
    spare = jnp.zeros((64, 128), jnp.float32)
    last_send[pl.ds(30, 64, stride=LAST), :] = spare
    last_send[pl.ds(31, 64, stride=LAST), :] = spare

    pl.semaphore_wait(barrier, PEERS - 1 + GROUPS - 1)
    send_waves(3)
    lax.fori_loop(5, 20, reorder, 0)
    for chunk in range(3):
        for step in (1, 2, 3):
            coeffs_copy(chunk, step).start()

    def waves_of(q):
        coeffs_all(q).wait_recv()
        e, f, h = (4, 3, 3) if q == 0 else (4, 3, 2) if q == 1 else (3, 4, 4)

        def one(r, carry):
            wave_row(
                (r, e),
                (0, 0, 0, 1),
                [piece(dx, q, r) for dx in (1, 2, 3)] + [piece(r + 1, q, e)],
                (3 + q, 6 + q, 9 + q, 3 * (r + 1) + q),
                waves_send.at[q],
                r * 10,
                ROWS,
            )
            return carry

        lax.fori_loop(0, 3, one, 0)
        wave_row(
            (f,) if f == h else (f, h),
            (0, 0, 0, 0) if f == h else (0, 0, 0, 1),
            [piece(dx, q, f) for dx in (1, 2, 3)] + [piece(None, 2, h)],
            (3 + q, 6 + q, 9 + q, 2),
            waves_send.at[q],
            30,
            ROWS,
        )

    waves_of(0)
    send_waves(0)
    waves_of(1)
    send_waves(1)
    waves_of(2)

    share = jnp.zeros((1, 128), jnp.float32)
    for group in range(12):
        row = jnp.sum(energy[group], axis=0, keepdims=True)
        for shift in (64, 32, 16, 8):
            row = row + pltpu.roll(row, shift, 1)
        share = jnp.where(lane // 8 == group, row, share)
    shares_send[0] = share
    shares[wide] = share

    def share_copy(i):
        return pltpu.make_async_remote_copy(
            src_ref=shares_send.at[0],
            dst_ref=shares.at[wide],
            send_sem=shares_send_sem,
            recv_sem=shares_sem,
            device_id={"grp": grp, "wide": partner(i)},
            device_id_type=MESH,
        )

    def send_share(i, carry):
        share_copy(i).start()
        return carry

    lax.fori_loop(0, PEERS - 1, send_share, 0)
    send_waves(2)

    def cosine(phase):
        phase = phase - LON * jnp.floor(phase * (1.0 / LON) + 0.5)
        angle = (LON // 4 - jnp.abs(phase)) * (2.0 * math.pi / LON)
        square = angle * angle
        series = 1.0 / 6227020800.0
        for term in (-1.0 / 39916800.0, 1.0 / 362880.0, -1.0 / 5040.0, 1.0 / 120.0, -1.0 / 6.0, 1.0):
            series = series * square + term
        return series * angle

    column = lax.broadcasted_iota(jnp.int32, (64, 128), 1)

    def spread_pairs(i, carry):
        for slot in range(5):
            pairs_down[pl.ds(slot * 64 + i, 1), :] = jnp.full((1, 128), pair[i * 5 + slot])
        return carry

    lax.fori_loop(0, PEERS, spread_pairs, 0)

    def make_synthesis(i, carry):
        parity, slot = i // 5, i % 5
        p = pairs_down[pl.ds(pl.multiple_of(slot * 64, 64), 64), :]
        number = jnp.where(p % 2 == parity, p, WAVES - 1 - p)
        factor = jnp.where(number == 0, 1.0, 2.0)
        cos_row = pl.multiple_of(slot * 64 + (slot // 4) * 256, 64)
        sin_row = pl.multiple_of(256 + slot * 64 + (slot // 4) * 64, 64)
        for tile in range(5):
            phase = (number * (column + tile * 128)).astype(jnp.float32)
            lanes = pl.ds(tile * 128, 128)
            high, low = split(factor * cosine(phase))
            synth_high[parity, pl.ds(cos_row, 64), lanes] = high
            synth_low[parity, pl.ds(cos_row, 64), lanes] = low
            high, low = split(-factor * cosine(phase - LON // 4))
            synth_high[parity, pl.ds(sin_row, 64), lanes] = high
            synth_low[parity, pl.ds(sin_row, 64), lanes] = low
        return carry

    lax.fori_loop(0, 10, make_synthesis, 0)

    def place_of(q, dx, slot):
        if dx == 0 and q < 2:
            return {0: (3, 0, q), 1: (3, 1, q), 2: (3, 2, q), 3: (3, 2, 2 + q), 4: (3, q, 3)}[slot]
        if dx == 0:
            return {0: (3, 0, 2), 1: (3, 1, 2), 2: (1, 3, 3), 3: (0, 3, 3), 4: (2, 3, 3)}[slot]
        e, f = (4, 3) if q < 2 else (3, 4)
        if slot == e:
            return (q, dx - 1, 3)
        return (q, 3 if slot == f else slot, dx - 1)

    def gather(q, messages):
        def turn(lat, carry):
            turned = {}
            for dx in range(GROUPS):
                group = lax.rem(grp + dx, GROUPS)
                rows = pl.ds(pl.multiple_of(lat * 32 + group * 8, 8), 8)
                for slot in range(5):
                    message, row, place = place_of(q, dx, slot)
                    if message not in messages:
                        continue
                    if (message, row) not in turned:
                        if message < 3:
                            value = waves[message, pl.ds(row * 10 + lat, 64, stride=ROWS), :]
                        else:
                            value = last[pl.ds(row * 10 + lat, 64, stride=LAST), :]
                        turned[message, row] = value.T
                    for parity in range(2):
                        for c in range(2):
                            at = place * 32 + parity * 16 + c * 8
                            column = c * 256 + slot * 64 if slot < 4 else 512 + c * 64
                            left[parity, rows, column : column + 64] = turned[message, row][
                                at : at + 8
                            ]
            return carry

        lax.fori_loop(0, 10, turn, 0)

    def synthesis(q):
        def part(i, carry):
            rows = pl.ds(pl.multiple_of(i * 32, 32), 32)
            for parity in range(2):
                high, low = split(left[parity, rows, :])
                left_high[parity, rows, :] = high
                left_low[parity, rows, :] = low
            return carry

        lax.fori_loop(0, 10, part, 0)

        def dot(a, b):
            return jnp.dot(a, b, preferred_element_type=jnp.float32)

        for start, width in ((0, 256), (256, 256), (512, 128)):
            halves = []
            for parity in range(2):
                right_high = synth_high[parity, :, start : start + width]
                right_low = synth_low[parity, :, start : start + width]
                halves.append(
                    dot(left_high[parity], right_high)
                    + dot(left_high[parity], right_low)
                    + dot(left_low[parity], right_high)
                )
            for value, offset in ((halves[0] + halves[1], 0), (halves[0] - halves[1], HALF)):
                for lat in range(10):
                    place = lat + south * (9 - 2 * lat)
                    for g in range(GROUPS):
                        for j in range(2):
                            row = lat * 32 + g * 8 + j * 4
                            level = g * 12 + q * 4
                            grid[
                                j,
                                place,
                                level : level + 4,
                                offset + start : offset + start + width,
                            ] = value[row : row + 4]

    wave_all(3).wait_recv()
    wave_all(0).wait_recv()

    def sums_copy(step):
        dest = other_group(step)
        return pltpu.make_async_remote_copy(
            src_ref=sums.at[grp],
            dst_ref=sums.at[grp],
            send_sem=sums_send_sem,
            recv_sem=sums_sem,
            device_id={"grp": dest, "wide": wide},
            device_id_type=MESH,
        )

    gather(0, (3, 0))
    synthesis(0)
    wave_all(1).wait_recv()
    gather(1, (3, 1))
    synthesis(1)
    gather(2, (3, 0, 1))

    shares_all = pltpu.make_async_remote_copy(
        src_ref=shares.at[pl.ds(0, PEERS - 1)],
        dst_ref=shares.at[pl.ds(0, PEERS - 1)],
        send_sem=shares_send_sem,
        recv_sem=shares_sem,
        device_id={"grp": grp, "wide": partner(0)},
        device_id_type=MESH,
    )
    shares_all.wait_send()
    shares_all.wait_recv()
    sums[grp] = jnp.broadcast_to(jnp.sum(shares[...], axis=0), (8, 128))
    for step in (1, 2, 3):
        sums_copy(step).start()
    sums_all = pltpu.make_async_remote_copy(
        src_ref=sums.at[0:3],
        dst_ref=sums.at[0:3],
        send_sem=sums_send_sem,
        recv_sem=sums_sem,
        device_id={"grp": other_group(1), "wide": wide},
        device_id_type=MESH,
    )
    sums_all.wait_send()
    sums_all.wait_recv()
    for group in range(GROUPS):
        row = sums[group, 0:1, :] * (1.0 / LAT)
        for j in range(2):
            placed = jnp.zeros((1, 128), jnp.float32)
            for step in range(GROUPS):
                for q in range(3):
                    source = (step * 3 + q) * 8 + j * 4
                    sink = ((group + step) % GROUPS) * 12 + q * 4
                    moved = pltpu.roll(row, (sink - source) % 128, 1) if sink != source else row
                    placed = jnp.where((lane >= sink) & (lane < sink + 4), moved, placed)
            sums_out[2 * group + j : 2 * group + j + 1, :] = placed[:, 0:48]
    wave_all(2).wait_recv()
    gather(2, (2,))
    synthesis(2)
    for chunk in range(3):
        coeffs_all(chunk).wait_send()
    for chunk in range(4):
        wave_all(chunk).wait_send()


def put_out(grid, sums, out, sums_out, sem):
    copies = [pltpu.make_async_copy(grid.at[j], out.at[j], sem.at[j]) for j in range(2)]
    for copy in copies:
        copy.start()
    sums_out[...] = sums[...]
    for copy in copies:
        copy.wait()


def local(spectral, legendre, pair_table, field_map):
    table = jnp.swapaxes(legendre, 1, 2)
    smem = pl.BlockSpec(memory_space=pltpu.SMEM)
    vmem = pl.BlockSpec(memory_space=pltpu.VMEM)
    hbm = pl.BlockSpec(memory_space=pltpu.HBM)
    dma = pltpu.SemaphoreType.DMA
    grid, sums = pl.pallas_call(
        kernel,
        name="transform",
        out_shape=(
            jax.ShapeDtypeStruct((2, 10, 48, LON), jnp.float32),
            jax.ShapeDtypeStruct((8, 48), jnp.float32),
        ),
        in_specs=[smem, smem, vmem, hbm],
        out_specs=(vmem, vmem),
        scratch_shapes=[
            pltpu.VMEM((5, 320, 641), jnp.float32),
            pltpu.VMEM((6, 5, 320, 128), jnp.float32),
            pltpu.VMEM((320, 128), jnp.int32),
            pltpu.VMEM((5, 320, 768), jnp.bfloat16),
            pltpu.VMEM((5, 320, 768), jnp.bfloat16),
            pltpu.VMEM((GROUPS, 15, 16, 768), jnp.float32),
            pltpu.VMEM((GROUPS, 15, 16, 768), jnp.float32),
            pltpu.VMEM((3, PEERS * ROWS, 128), jnp.float32),
            pltpu.VMEM((PEERS * LAST, 128), jnp.float32),
            pltpu.VMEM((3, PEERS * ROWS, 128), jnp.float32),
            pltpu.VMEM((PEERS * LAST, 128), jnp.float32),
            pltpu.VMEM((2, HALF, HALF), jnp.bfloat16),
            pltpu.VMEM((2, HALF, HALF), jnp.bfloat16),
            pltpu.VMEM((2, 320, HALF), jnp.bfloat16),
            pltpu.VMEM((2, 320, HALF), jnp.bfloat16),
            pltpu.VMEM((2, 320, HALF), jnp.float32),
            pltpu.VMEM((12, 8, 128), jnp.float32),
            pltpu.VMEM((1, 1, 128), jnp.float32),
            pltpu.VMEM((PEERS, 1, 128), jnp.float32),
            pltpu.VMEM((GROUPS, 8, 128), jnp.float32),
            dma((6,)),
            dma((3,)),
            dma((3,)),
            dma((4,)),
            dma((4,)),
            dma,
            dma,
            dma,
            dma,
        ],
        compiler_params=pltpu.CompilerParams(
            collective_id=0, has_side_effects=True, vmem_limit_bytes=46 * 2**20
        ),
    )(pair_table, field_map, spectral, table)
    grid, checksums = pl.pallas_call(
        put_out,
        name="put_out",
        out_shape=(
            jax.ShapeDtypeStruct((2, 10, 48, LON), jnp.float32),
            jax.ShapeDtypeStruct((8, 48), jnp.float32),
        ),
        in_specs=[vmem, vmem],
        out_specs=(hbm, vmem),
        scratch_shapes=[dma((2,))],
        compiler_params=pltpu.CompilerParams(vmem_limit_bytes=2**20),
    )(grid, sums)
    return jnp.swapaxes(grid, 1, 2), checksums


def solution(mesh):
    placed = (P(None, "grp", "wide", None, None), P("wide", None, None), P(), P())
    return jax.shard_map(
        local,
        mesh=mesh,
        in_specs=placed,
        out_specs=(P("grp", None, "wide", None), P()),
        check_vma=False,
    )
```

```python
import functools
import math

import jax
import jax.numpy as jnp
from jax import lax
from jax.experimental import pallas as pl
from jax.experimental.pallas import tpu as pltpu
from jax.sharding import PartitionSpec as P

WAVES = 640
LAT = 640
LON = 1280
HALF = LON // 2
MESH = pl.DeviceIdType.MESH
ROWS = 40
LAST = 32
GROUPS = 4
PEERS = 64


def split(value):
    high = value.astype(jnp.bfloat16)
    low = (value - high.astype(jnp.float32)).astype(jnp.bfloat16)
    return high, low


def kernel(
    pair,
    fields,
    spectral_hbm,
    table_hbm,
    grid,
    sums_out,
    spectral,
    table_whole,
    table,
    pairs_down,
    table_high,
    table_low,
    coeffs_send,
    coeffs,
    waves_send,
    last_send,
    waves,
    last,
    synth_high,
    synth_low,
    left_high,
    left_low,
    left,
    energy,
    shares_send,
    shares,
    sums,
    first_sem,
    table_sem,
    coeffs_send_sem,
    coeffs_sem,
    waves_send_sem,
    waves_sem,
    shares_send_sem,
    shares_sem,
    sums_send_sem,
    sums_sem,
):
    grp = lax.axis_index("grp")
    wide = lax.axis_index("wide")
    my_y, my_z, my_c = wide // 16, (wide // 2) % 8, wide % 2
    south = wide // 32

    def other_group(step):
        return lax.rem(grp + step, GROUPS)

    def partner(i):
        k = i % 8
        up = (k + 2) // 2
        dz = (k % 2) * (8 - up) + (1 - k % 2) * up
        dz = (1 - k // 6) * dz + (k // 6) * (1 - k % 2) * 4
        dy = 3 - (i // 8) % 4
        dc = 1 - i // 32
        return (
            lax.rem(my_y + dy, 4) * 16 + lax.rem(my_z + dz, 8) * 2 + lax.rem(my_c + dc, 2)
        )

    def block_of(dest):
        return dest + (dest // 32) * (95 - 2 * dest)

    barrier = pltpu.get_barrier_semaphore()
    first_copies = [
        pltpu.make_async_copy(source, sink, first_sem.at[i])
        for i, (source, sink) in enumerate(((spectral_hbm, spectral),))
    ]
    for copy in first_copies:
        copy.start()
    table_copies = [
        pltpu.make_async_copy(
            table_hbm.at[:, :, tile * 128 : (tile + 1) * 128],
            table.at[tile],
            table_sem.at[tile],
        )
        for tile in range(5)
    ] + [pltpu.make_async_copy(table_hbm, table_whole, table_sem.at[5])]
    for copy in table_copies:
        copy.start()

    def greet(i, carry):
        pl.semaphore_signal(
            barrier, inc=1, device_id={"grp": grp, "wide": partner(i)}, device_id_type=MESH
        )
        return carry

    lax.fori_loop(0, PEERS - 1, greet, 0)
    for step in (1, 2, 3):
        pl.semaphore_signal(
            barrier,
            inc=1,
            device_id={"grp": other_group(step), "wide": wide},
            device_id_type=MESH,
        )

    coeffs_send[:, :, :, 640:768] = jnp.zeros((GROUPS, 15, 16, 128), jnp.float32)

    def reorder(i, carry):
        group, slot = lax.rem(grp + i // 5, GROUPS), i % 5
        for j in range(2):
            field = fields[2 * group + j]
            for level in range(12):
                q, l = level // 4, level % 4
                for c in range(2):
                    coeffs_send[group, q * 5 + slot, c * 8 + j * 4 + l, 0:641] = spectral[
                        field, level, slot, c, :
                    ]
        return carry

    for copy in first_copies:
        copy.wait()
    lax.fori_loop(0, 5, reorder, 0)

    def coeffs_copy(chunk, step):
        blocks = pl.ds(chunk * 5, 5)
        dest = other_group(step)
        return pltpu.make_async_remote_copy(
            src_ref=coeffs_send.at[dest, blocks],
            dst_ref=coeffs.at[grp, blocks],
            send_sem=coeffs_send_sem.at[chunk],
            recv_sem=coeffs_sem.at[chunk],
            device_id={"grp": dest, "wide": wide},
            device_id_type=MESH,
        )

    def coeffs_all(chunk):
        blocks = pl.ds(chunk * 5, 5)
        return pltpu.make_async_remote_copy(
            src_ref=coeffs_send.at[0:3, blocks],
            dst_ref=coeffs.at[0:3, blocks],
            send_sem=coeffs_send_sem.at[chunk],
            recv_sem=coeffs_sem.at[chunk],
            device_id={"grp": other_group(1), "wide": wide},
            device_id_type=MESH,
        )

    for copy in table_copies:
        copy.wait()
    first_lane = lax.broadcasted_iota(jnp.int32, (320, 128), 1) == 0

    def part_end(slot, carry):
        table[5, slot] = jnp.where(first_lane, table_whole[slot, :, 640:641], 0.0)
        return carry

    lax.fori_loop(0, 5, part_end, 0)

    def part_table(i, carry):
        slot, lat = i // 10, i % 10
        rows = pl.ds(pl.multiple_of(lat * 32, 32), 32)
        for tile in range(6):
            value = table[tile, slot, pl.ds(lat, 32, stride=10), :]
            high, low = split(value)
            table_high[slot, rows, tile * 128 : (tile + 1) * 128] = high
            table_low[slot, rows, tile * 128 : (tile + 1) * 128] = low
        return carry

    lax.fori_loop(0, 50, part_table, 0)

    energy[...] = jnp.zeros_like(energy)
    degree = lax.broadcasted_iota(jnp.int32, (1, 768), 1)
    lane = lax.broadcasted_iota(jnp.int32, (1, 128), 1)

    def masks(slot):
        p = pair[wide * 5 + slot]
        boundary = WAVES - p
        first_part = degree < boundary
        start = jnp.where(first_part, 0, boundary)
        sign = 1.0 - 2.0 * ((degree - start) % 2).astype(jnp.float32)
        is_first = first_part.astype(jnp.float32)
        inside = (degree <= WAVES).astype(jnp.float32)
        odd = (p % 2).astype(jnp.float32)
        even_mask = (is_first * (1.0 - odd) + (1.0 - is_first) * odd) * inside
        odd_mask = (1.0 - even_mask) * inside
        return p, even_mask, odd_mask, sign

    def piece(dx, q, slot):
        if dx is None:
            return coeffs_send[grp, q * 5 + slot]
        return coeffs[lax.rem(grp + dx, GROUPS), q * 5 + slot]

    nt = (((1,), (1,)), ((), ()))

    def dot_nt(a, b):
        return lax.dot_general(a, b, nt, preferred_element_type=jnp.float32)

    def wave_row(slots, members, tiles, groups, target, first_row, stride):
        result = None
        zero = jnp.zeros((1, 128), jnp.float32)
        empty = jnp.zeros((32, 768), jnp.float32)
        for number, slot in enumerate(slots):
            p, even_mask, odd_mask, sign = masks(slot)
            north, southern = [], []
            for i in range(4):
                if members[i] == number:
                    parts = jnp.concatenate([tiles[i] * even_mask, tiles[i] * odd_mask], 0)
                    north.append(parts)
                    southern.append(parts * sign)
                    here = (lane // 32 == i) & (lane % 32 < 16)
                    zero = zero + jnp.where(p == 0, 1.0, 0.0) * here.astype(jnp.float32)
                else:
                    north.append(empty)
                    southern.append(empty)
            right_high, right_low = split(jnp.concatenate(north + southern, 0))
            high = table_high[slot]
            product = (
                dot_nt(high, right_high) + dot_nt(high, right_low) + dot_nt(table_low[slot], right_high)
            )
            result = product if result is None else result + product
        for lat in range(10):
            rows = result[lat * 32 : (lat + 1) * 32]
            target[pl.ds(first_row + lat, 32, stride=stride), :] = rows[:, 0:128]
            target[pl.ds(first_row + lat + 32 * stride, 32, stride=stride), :] = rows[:, 128:256]
        squares = result * result
        squares = squares[:, 0:128] + squares[:, 128:256]
        total = jnp.sum(squares.reshape(40, 8, 128), axis=0)
        real = 1.0 - ((lane // 8) % 2).astype(jnp.float32)
        total = total * (2.0 * (1.0 - zero) + real * zero)
        for i in range(4):
            energy[groups[i]] = energy[groups[i]] + total * (lane // 32 == i).astype(jnp.float32)

    def wave_copy(chunk, i):
        dest = partner(i)
        size = ROWS if chunk < 3 else LAST
        source = waves_send.at[chunk] if chunk < 3 else last_send
        sink = waves.at[chunk] if chunk < 3 else last
        return pltpu.make_async_remote_copy(
            src_ref=source.at[pl.ds(pl.multiple_of(block_of(dest) * size, 8), size)],
            dst_ref=sink.at[pl.ds(pl.multiple_of(wide * size, 8), size)],
            send_sem=waves_send_sem.at[chunk],
            recv_sem=waves_sem.at[chunk],
            device_id={"grp": grp, "wide": dest},
            device_id_type=MESH,
        )

    def wave_all(chunk):
        size = ROWS if chunk < 3 else LAST
        source = waves_send.at[chunk] if chunk < 3 else last_send
        sink = waves.at[chunk] if chunk < 3 else last
        return pltpu.make_async_remote_copy(
            src_ref=source.at[pl.ds(0, (PEERS - 1) * size)],
            dst_ref=sink.at[pl.ds(0, (PEERS - 1) * size)],
            send_sem=waves_send_sem.at[chunk],
            recv_sem=waves_sem.at[chunk],
            device_id={"grp": grp, "wide": partner(0)},
            device_id_type=MESH,
        )

    def send_waves(chunk):
        def one(i, carry):
            wave_copy(chunk, i).start()
            return carry

        lax.fori_loop(0, PEERS - 1, one, 0)
        size = ROWS if chunk < 3 else LAST
        source = waves_send.at[chunk] if chunk < 3 else last_send
        sink = waves.at[chunk] if chunk < 3 else last
        sink[pl.ds(pl.multiple_of(wide * size, 8), size), :] = source[
            pl.ds(pl.multiple_of(block_of(wide) * size, 8), size), :
        ]

    def own_row(r, carry):
        wave_row(
            (r, 4),
            (0, 0, 0, 1),
            [piece(None, q, r) for q in range(3)] + [piece(None, r, 4)],
            (0, 1, 2, r),
            last_send,
            r * 10,
            LAST,
        )
        return carry

    lax.fori_loop(0, 2, own_row, 0)
    wave_row(
        (2, 3),
        (0, 0, 1, 1),
        [piece(None, 0, 2), piece(None, 1, 2), piece(None, 0, 3), piece(None, 1, 3)],
        (0, 1, 0, 1),
        last_send,
        20,
        LAST,
    )
    spare = jnp.zeros((64, 128), jnp.float32)
    last_send[pl.ds(30, 64, stride=LAST), :] = spare
    last_send[pl.ds(31, 64, stride=LAST), :] = spare

    pl.semaphore_wait(barrier, PEERS - 1 + GROUPS - 1)
    send_waves(3)
    lax.fori_loop(5, 20, reorder, 0)
    for chunk in range(3):
        for step in (1, 2, 3):
            coeffs_copy(chunk, step).start()

    def waves_of(q):
        coeffs_all(q).wait_recv()
        e, f, h = (4, 3, 3) if q == 0 else (4, 3, 2) if q == 1 else (3, 4, 4)

        def one(r, carry):
            wave_row(
                (r, e),
                (0, 0, 0, 1),
                [piece(dx, q, r) for dx in (1, 2, 3)] + [piece(r + 1, q, e)],
                (3 + q, 6 + q, 9 + q, 3 * (r + 1) + q),
                waves_send.at[q],
                r * 10,
                ROWS,
            )
            return carry

        lax.fori_loop(0, 3, one, 0)
        wave_row(
            (f,) if f == h else (f, h),
            (0, 0, 0, 0) if f == h else (0, 0, 0, 1),
            [piece(dx, q, f) for dx in (1, 2, 3)] + [piece(None, 2, h)],
            (3 + q, 6 + q, 9 + q, 2),
            waves_send.at[q],
            30,
            ROWS,
        )

    waves_of(0)
    send_waves(0)
    waves_of(1)
    send_waves(1)
    waves_of(2)

    share = jnp.zeros((1, 128), jnp.float32)
    for group in range(12):
        row = jnp.sum(energy[group], axis=0, keepdims=True)
        for shift in (64, 32, 16, 8):
            row = row + pltpu.roll(row, shift, 1)
        share = jnp.where(lane // 8 == group, row, share)
    shares_send[0] = share
    shares[wide] = share

    def share_copy(i):
        return pltpu.make_async_remote_copy(
            src_ref=shares_send.at[0],
            dst_ref=shares.at[wide],
            send_sem=shares_send_sem,
            recv_sem=shares_sem,
            device_id={"grp": grp, "wide": partner(i)},
            device_id_type=MESH,
        )

    def send_share(i, carry):
        share_copy(i).start()
        return carry

    lax.fori_loop(0, PEERS - 1, send_share, 0)
    send_waves(2)

    def cosine(phase):
        phase = phase - LON * jnp.floor(phase * (1.0 / LON) + 0.5)
        angle = (LON // 4 - jnp.abs(phase)) * (2.0 * math.pi / LON)
        square = angle * angle
        series = 1.0 / 6227020800.0
        for term in (-1.0 / 39916800.0, 1.0 / 362880.0, -1.0 / 5040.0, 1.0 / 120.0, -1.0 / 6.0, 1.0):
            series = series * square + term
        return series * angle

    column = lax.broadcasted_iota(jnp.int32, (64, 128), 1)

    def spread_pairs(i, carry):
        for slot in range(5):
            pairs_down[pl.ds(slot * 64 + i, 1), :] = jnp.full((1, 128), pair[i * 5 + slot])
        return carry

    lax.fori_loop(0, PEERS, spread_pairs, 0)

    def make_synthesis(i, carry):
        parity, slot = i // 5, i % 5
        p = pairs_down[pl.ds(pl.multiple_of(slot * 64, 64), 64), :]
        number = jnp.where(p % 2 == parity, p, WAVES - 1 - p)
        factor = jnp.where(number == 0, 1.0, 2.0)
        cos_row = pl.multiple_of(slot * 64 + (slot // 4) * 256, 64)
        sin_row = pl.multiple_of(256 + slot * 64 + (slot // 4) * 64, 64)
        for tile in range(5):
            phase = (number * (column + tile * 128)).astype(jnp.float32)
            lanes = pl.ds(tile * 128, 128)
            high, low = split(factor * cosine(phase))
            synth_high[parity, pl.ds(cos_row, 64), lanes] = high
            synth_low[parity, pl.ds(cos_row, 64), lanes] = low
            high, low = split(-factor * cosine(phase - LON // 4))
            synth_high[parity, pl.ds(sin_row, 64), lanes] = high
            synth_low[parity, pl.ds(sin_row, 64), lanes] = low
        return carry

    lax.fori_loop(0, 10, make_synthesis, 0)

    def place_of(q, dx, slot):
        if dx == 0 and q < 2:
            return {0: (3, 0, q), 1: (3, 1, q), 2: (3, 2, q), 3: (3, 2, 2 + q), 4: (3, q, 3)}[slot]
        if dx == 0:
            return {0: (3, 0, 2), 1: (3, 1, 2), 2: (1, 3, 3), 3: (0, 3, 3), 4: (2, 3, 3)}[slot]
        e, f = (4, 3) if q < 2 else (3, 4)
        if slot == e:
            return (q, dx - 1, 3)
        return (q, 3 if slot == f else slot, dx - 1)

    def gather(q, messages):
        def turn(lat, carry):
            turned = {}
            for dx in range(GROUPS):
                group = lax.rem(grp + dx, GROUPS)
                rows = pl.ds(pl.multiple_of(lat * 32 + group * 8, 8), 8)
                for slot in range(5):
                    message, row, place = place_of(q, dx, slot)
                    if message not in messages:
                        continue
                    if (message, row) not in turned:
                        if message < 3:
                            value = waves[message, pl.ds(row * 10 + lat, 64, stride=ROWS), :]
                        else:
                            value = last[pl.ds(row * 10 + lat, 64, stride=LAST), :]
                        turned[message, row] = value.T
                    for parity in range(2):
                        for c in range(2):
                            at = place * 32 + parity * 16 + c * 8
                            column = c * 256 + slot * 64 if slot < 4 else 512 + c * 64
                            left[parity, rows, column : column + 64] = turned[message, row][
                                at : at + 8
                            ]
            return carry

        lax.fori_loop(0, 10, turn, 0)

    def synthesis(q):
        def part(i, carry):
            rows = pl.ds(pl.multiple_of(i * 32, 32), 32)
            for parity in range(2):
                high, low = split(left[parity, rows, :])
                left_high[parity, rows, :] = high
                left_low[parity, rows, :] = low
            return carry

        lax.fori_loop(0, 10, part, 0)

        def dot(a, b):
            return jnp.dot(a, b, preferred_element_type=jnp.float32)

        for start, width in ((0, 256), (256, 256), (512, 128)):
            halves = []
            for parity in range(2):
                right_high = synth_high[parity, :, start : start + width]
                right_low = synth_low[parity, :, start : start + width]
                halves.append(
                    dot(left_high[parity], right_high)
                    + dot(left_high[parity], right_low)
                    + dot(left_low[parity], right_high)
                )
            for value, offset in ((halves[0] + halves[1], 0), (halves[0] - halves[1], HALF)):
                for lat in range(10):
                    place = lat + south * (9 - 2 * lat)
                    for g in range(GROUPS):
                        for j in range(2):
                            row = lat * 32 + g * 8 + j * 4
                            level = g * 12 + q * 4
                            grid[
                                j,
                                place,
                                level : level + 4,
                                offset + start : offset + start + width,
                            ] = value[row : row + 4]

    wave_all(3).wait_recv()
    wave_all(0).wait_recv()

    def sums_copy(step):
        dest = other_group(step)
        return pltpu.make_async_remote_copy(
            src_ref=sums.at[grp],
            dst_ref=sums.at[grp],
            send_sem=sums_send_sem,
            recv_sem=sums_sem,
            device_id={"grp": dest, "wide": wide},
            device_id_type=MESH,
        )

    gather(0, (3, 0))
    synthesis(0)
    wave_all(1).wait_recv()
    gather(1, (3, 1))
    synthesis(1)
    gather(2, (3, 0, 1))

    shares_all = pltpu.make_async_remote_copy(
        src_ref=shares.at[pl.ds(0, PEERS - 1)],
        dst_ref=shares.at[pl.ds(0, PEERS - 1)],
        send_sem=shares_send_sem,
        recv_sem=shares_sem,
        device_id={"grp": grp, "wide": partner(0)},
        device_id_type=MESH,
    )
    shares_all.wait_send()
    shares_all.wait_recv()
    sums[grp] = jnp.broadcast_to(jnp.sum(shares[...], axis=0), (8, 128))
    for step in (1, 2, 3):
        sums_copy(step).start()
    sums_all = pltpu.make_async_remote_copy(
        src_ref=sums.at[0:3],
        dst_ref=sums.at[0:3],
        send_sem=sums_send_sem,
        recv_sem=sums_sem,
        device_id={"grp": other_group(1), "wide": wide},
        device_id_type=MESH,
    )
    sums_all.wait_send()
    sums_all.wait_recv()
    for group in range(GROUPS):
        row = sums[group, 0:1, :] * (1.0 / LAT)
        for j in range(2):
            placed = jnp.zeros((1, 128), jnp.float32)
            for step in range(GROUPS):
                for q in range(3):
                    source = (step * 3 + q) * 8 + j * 4
                    sink = ((group + step) % GROUPS) * 12 + q * 4
                    moved = pltpu.roll(row, (sink - source) % 128, 1) if sink != source else row
                    placed = jnp.where((lane >= sink) & (lane < sink + 4), moved, placed)
            sums_out[2 * group + j : 2 * group + j + 1, :] = placed[:, 0:48]
    wave_all(2).wait_recv()
    gather(2, (2,))
    synthesis(2)
    for chunk in range(3):
        coeffs_all(chunk).wait_send()
    for chunk in range(4):
        wave_all(chunk).wait_send()


def put_out(grid, sums, out, sums_out, sem):
    copies = [
        pltpu.make_async_copy(
            grid.at[i // 5, pl.ds(i % 5 * 2, 2)], out.at[i // 5, pl.ds(i % 5 * 2, 2)], sem.at[i]
        )
        for i in range(10)
    ]
    for copy in copies:
        copy.start()
    sums_out[...] = sums[...]
    for copy in copies:
        copy.wait()


def local(spectral, legendre, pair_table, field_map):
    table = jnp.swapaxes(legendre, 1, 2)
    smem = pl.BlockSpec(memory_space=pltpu.SMEM)
    vmem = pl.BlockSpec(memory_space=pltpu.VMEM)
    hbm = pl.BlockSpec(memory_space=pltpu.HBM)
    dma = pltpu.SemaphoreType.DMA
    grid, sums = pl.pallas_call(
        kernel,
        name="transform",
        out_shape=(
            pltpu.VMEM((2, 10, 48, LON), jnp.float32),
            pltpu.VMEM((8, 48), jnp.float32),
        ),
        in_specs=[smem, smem, hbm, hbm],
        out_specs=(vmem, vmem),
        scratch_shapes=[
            pltpu.VMEM((8, 12, 5, 2, 641), jnp.float32),
            pltpu.VMEM((5, 320, 641), jnp.float32),
            pltpu.VMEM((6, 5, 320, 128), jnp.float32),
            pltpu.VMEM((320, 128), jnp.int32),
            pltpu.VMEM((5, 320, 768), jnp.bfloat16),
            pltpu.VMEM((5, 320, 768), jnp.bfloat16),
            pltpu.VMEM((GROUPS, 15, 16, 768), jnp.float32),
            pltpu.VMEM((GROUPS, 15, 16, 768), jnp.float32),
            pltpu.VMEM((3, PEERS * ROWS, 128), jnp.float32),
            pltpu.VMEM((PEERS * LAST, 128), jnp.float32),
            pltpu.VMEM((3, PEERS * ROWS, 128), jnp.float32),
            pltpu.VMEM((PEERS * LAST, 128), jnp.float32),
            pltpu.VMEM((2, HALF, HALF), jnp.bfloat16),
            pltpu.VMEM((2, HALF, HALF), jnp.bfloat16),
            pltpu.VMEM((2, 320, HALF), jnp.bfloat16),
            pltpu.VMEM((2, 320, HALF), jnp.bfloat16),
            pltpu.VMEM((2, 320, HALF), jnp.float32),
            pltpu.VMEM((12, 8, 128), jnp.float32),
            pltpu.VMEM((1, 1, 128), jnp.float32),
            pltpu.VMEM((PEERS, 1, 128), jnp.float32),
            pltpu.VMEM((GROUPS, 8, 128), jnp.float32),
            dma((3,)),
            dma((6,)),
            dma((3,)),
            dma((3,)),
            dma((4,)),
            dma((4,)),
            dma,
            dma,
            dma,
            dma,
        ],
        compiler_params=pltpu.CompilerParams(
            collective_id=0, has_side_effects=True, vmem_limit_bytes=50 * 2**20
        ),
    )(pair_table, field_map, spectral, table)
    grid, checksums = pl.pallas_call(
        put_out,
        name="put_out",
        out_shape=(
            jax.ShapeDtypeStruct((2, 10, 48, LON), jnp.float32),
            jax.ShapeDtypeStruct((8, 48), jnp.float32),
        ),
        in_specs=[vmem, vmem],
        out_specs=(hbm, vmem),
        scratch_shapes=[dma((10,))],
        compiler_params=pltpu.CompilerParams(vmem_limit_bytes=2**20),
    )(grid, sums)
    return jnp.swapaxes(grid, 1, 2), checksums


def solution(mesh):
    placed = (P(None, "grp", "wide", None, None), P("wide", None, None), P(), P())
    return jax.shard_map(
        local,
        mesh=mesh,
        in_specs=placed,
        out_specs=(P("grp", None, "wide", None), P()),
        check_vma=False,
    )
```
